32 devices in a mesh: items: 8 (over y, x, core), heads: 4 (over z).
Axes of the slice: x: 2, y: 2, z: 4, core: 2. Of those that a mesh axis runs over, the one named last changes fastest.
Arguments:
- tokens: bfloat16 [16, 1280, 768], P('items', 'heads'), may hold values from -6 to 6
- passes: int32 [16], P('items'), may hold values from 2 to 5, as said below
- embed: bfloat16 [5, 768], replicated, may hold values from -3 to 3
- gain_one: bfloat16 [768], replicated, may hold values from 0.5 to 1.5
- w_qkv: bfloat16 [768, 2304], replicated, may hold values from -0.3125 to 0.3125
- w_out: bfloat16 [768, 768], replicated, may hold values from -2 to 2
- gain_two: bfloat16 [768], replicated, may hold values from 0.5 to 1.5
- w_up: bfloat16 [768, 3072], replicated, may hold values from -0.21875 to 0.21875
- w_down: bfloat16 [3072, 768], replicated, may hold values from -0.109375 to 0.109375
- cotangent: bfloat16 [16, 1280, 768], P('items', 'heads'), may hold values from -6 to 6
Outputs:
- outputs: bfloat16 [16, 1280, 768], P('items', 'heads')
- grad_tokens: bfloat16 [16, 1280, 768], P('items', 'heads')
- grad_embed: float32 [5, 768], P(None, 'heads')
- grad_gain_one: float32 [768], P('heads')
- grad_w_qkv: float32 [768, 2304], P('heads')
- grad_w_out: float32 [768, 768], P('heads')
- grad_gain_two: float32 [768], P('heads')
- grad_w_up: float32 [768, 3072], P('heads')
- grad_w_down: float32 [3072, 768], P('heads')
The draws below stay inside these ranges and needn't reach their ends.
Inputs may be any that keep to these rules, and one draw needn't show every extreme that they name: Each item's number of passes; every draw holds an item with 2 passes and one with 5.
All inputs are finite; a program needn't handle non-finite values.
Results may differ from the reference program's by a relative error of at most 0.013.
Values may be sent and summed in bfloat16 or wider, within the bound.
A program may use at most 192 MiB of HBM per device.

```python
import jax
import jax.numpy as jnp
from jax import lax

D = 768
HEADS = 12
HEAD_DIM = 64
FF = 3072
PASSES_MAX = 5
TOK_PASS = 256
LEN = 1280
ITEMS = 16


def draw_passes(key, part):
    key_base, key_high, key_shift = jax.random.split(key, 3)
    counts = jax.random.randint(key_base, (ITEMS,), 2, PASSES_MAX + 1)
    high_item = jax.random.randint(key_high, (), 0, ITEMS)
    shift_by = jax.random.randint(key_shift, (), 1, ITEMS)
    low_item = (high_item + shift_by) % ITEMS
    counts = counts.at[high_item].set(PASSES_MAX)
    counts = counts.at[low_item].set(2)
    return counts.astype(jnp.int32)


def block_scale(own_key, dims, cuts, low, top_value):
    level, own = 1.0, jax.random.fold_in(own_key, 6)
    for axis_at, parts in cuts:
        draws = jnp.exp(jax.random.uniform(jax.random.fold_in(own, axis_at), (parts,), jnp.float32, low / len(cuts), top_value / len(cuts)))
        level = level * jnp.repeat(draws, dims[axis_at] // parts).reshape([-1 if axis == axis_at else 1 for axis in range(len(dims))])
    return level


def bell_draw(own_key, dims, scale, most, cuts=(), held_as=jnp.bfloat16):
    level = block_scale(own_key, dims, cuts, -0.22, 0.18) if cuts else 1.0
    drawn = jax.random.normal(own_key, dims, jnp.float32) * scale * level
    return jnp.minimum(jnp.maximum(drawn, -most), most).astype(held_as)


def setup_inputs(seed: int = 0) -> dict:
    arg_keys = jax.random.split(jax.random.key(seed), 11)
    tokens = bell_draw(arg_keys[0], (ITEMS, LEN, D), 1.0, 6.0, ((0, 8), (1, 4)))
    passes = draw_passes(jax.random.fold_in(arg_keys[10], 71), 0)
    embed = bell_draw(arg_keys[2], (PASSES_MAX, D), 0.5, 3.0)
    gain_one = jnp.clip(1.0 + 0.1 * jax.random.normal(arg_keys[3], (D,), jnp.float32), 0.5, 1.5).astype(jnp.bfloat16)
    w_qkv = bell_draw(arg_keys[4], (D, 3 * D), (D // 2) ** -0.5, 0.3125)
    w_out = bell_draw(arg_keys[5], (D, D), 8 ** -0.5, 2.0)
    gain_two = jnp.clip(1.0 + 0.1 * jax.random.normal(arg_keys[6], (D,), jnp.float32), 0.5, 1.5).astype(jnp.bfloat16)
    w_up = bell_draw(arg_keys[7], (D, FF), D ** -0.5, 0.21875)
    w_down = bell_draw(arg_keys[8], (FF, D), FF ** -0.5, 0.109375)
    cotangent = bell_draw(arg_keys[9], (ITEMS, LEN, D), 1.0, 6.0, ((0, 8), (1, 4)))
    return {"tokens": tokens, "passes": passes, "embed": embed, "gain_one": gain_one, "w_qkv": w_qkv, "w_out": w_out, "gain_two": gain_two, "w_up": w_up, "w_down": w_down, "cotangent": cotangent}


@jax.custom_vjp
def low(v):
    return lax.optimization_barrier(v.astype(jnp.bfloat16)).astype(jnp.float32)

@jax.custom_vjp
def low_back(v):
    return v

def low_keep(v):
    return (low(v), None)

def low_pass(kept, grad):
    return (grad,)

def back_keep(v):
    return (v, None)

def back_low(kept, grad):
    return (low(grad),)
low.defvjp(low_keep, low_pass)
low_back.defvjp(back_keep, back_low)
highest = lax.Precision.HIGHEST
epsilon = 1e-05
masked_fill = -1e+30

def layer_norm(values_in, gain):
    centered = values_in - lax.optimization_barrier(jnp.mean(values_in, axis=-1, keepdims=True))
    spread = lax.optimization_barrier(jnp.mean(centered * centered, axis=-1, keepdims=True))
    return centered * lax.rsqrt(spread + epsilon) * gain

def item_forward(params, x_item, pass_count):
    w_qkv, w_out, w_up, w_down, gain_one, gain_two, embed = params
    slot_index = jnp.arange(LEN, dtype=jnp.int32)
    is_valid = slot_index < TOK_PASS * pass_count
    pass_index = slot_index % pass_count
    onehot = (pass_index[:, None] == jnp.arange(PASSES_MAX, dtype=jnp.int32)[None, :]).astype(jnp.float32)
    hidden = x_item + jnp.dot(onehot, embed, precision=highest)
    normed = low(layer_norm(hidden, gain_one))
    qkv_rows = jnp.dot(normed, w_qkv, precision=highest)
    queries = low(low_back(qkv_rows[:, :D])).reshape(LEN, HEADS, HEAD_DIM)
    keys_all = low(low_back(qkv_rows[:, D:2 * D])).reshape(LEN, HEADS, HEAD_DIM)
    values_all = low(low_back(qkv_rows[:, 2 * D:])).reshape(LEN, HEADS, HEAD_DIM)
    scores = low_back(jnp.einsum('qhd,khd->hqk', queries, keys_all, precision=highest) * HEAD_DIM ** (-0.5))
    allowed = (slot_index[None, :] <= slot_index[:, None]) & is_valid[None, :]
    masked = jnp.where(allowed[None], scores, masked_fill)
    row_max = lax.optimization_barrier(jnp.max(masked, axis=-1, keepdims=True))
    exp_scores = jnp.exp(masked - row_max)
    prob_low = low(exp_scores / lax.optimization_barrier(jnp.sum(exp_scores, axis=-1, keepdims=True)))
    mixed_out = jnp.einsum('hqk,khd->qhd', prob_low, values_all, precision=highest)
    mixed_out = low(low_back(mixed_out)).reshape(LEN, D)
    branch = low_back(jnp.dot(mixed_out, w_out, precision=highest))
    middle = hidden + branch
    second = low(layer_norm(middle, gain_two))
    up_proj = low_back(jnp.dot(second, w_up, precision=highest))
    active = low(jax.nn.gelu(up_proj, approximate=True))
    result = middle + low_back(jnp.dot(active, w_down, precision=highest))
    return result * is_valid.astype(jnp.float32)[:, None]

def reference(tokens, passes, embed, gain_one, w_qkv, w_out, gain_two, w_up, w_down, cotangent):
    params = tuple((weight.astype(jnp.float32) for weight in (w_qkv, w_out, w_up, w_down, gain_one, gain_two, embed)))
    zero_grads = tuple((jnp.zeros_like(weight) for weight in params))

    def one_item(running, inputs):
        x_item, pass_count, cot_item = inputs

        def forward(weights, x_rows):
            return item_forward(weights, x_rows, pass_count)
        out_item, pullback = jax.vjp(forward, params, x_item.astype(jnp.float32))
        grads, grad_x = pullback(cot_item.astype(jnp.float32))
        running = tuple((left + right for left, right in zip(running, grads)))
        return (running, (out_item.astype(jnp.bfloat16), grad_x.astype(jnp.bfloat16)))
    totals, (outputs, grad_tokens) = lax.scan(one_item, zero_grads, (tokens, passes, cotangent))
    grad_qkv, grad_out, grad_up, grad_down, grad_one, grad_two, grad_embed = totals
    return (outputs, grad_tokens, grad_embed, grad_one, grad_qkv, grad_out, grad_two, grad_up, grad_down)
```

```python
import jax
import jax.numpy as jnp
from jax import lax
from jax.experimental import pallas as pl
from jax.experimental.pallas import tpu as pltpu
from jax.sharding import PartitionSpec as P

HEADS = 12
HEAD_DIM = 64
PASSES_MAX = 5
TOK_PASS = 256

epsilon = 1e-05
masked_fill = -1e30
BF16 = jnp.bfloat16
F32 = jnp.float32
NT = (((1,), (1,)), ((), ()))
VMEM_LIMIT = 56 * 1024 * 1024


def matmul(left, right):
    return jnp.dot(left, right, preferred_element_type=F32)


def layer_norm(values_in, gain):
    centered = values_in - jnp.mean(values_in, axis=-1, keepdims=True)
    spread = jnp.mean(centered * centered, axis=-1, keepdims=True)
    return centered * lax.rsqrt(spread + epsilon) * gain


def gelu_tanh(values_in):
    return jax.nn.gelu(values_in, approximate=True)


def causal(scores_t, block):
    shape = (block, block)
    allowed = lax.broadcasted_iota(jnp.int32, shape, 0) <= lax.broadcasted_iota(jnp.int32, shape, 1)
    return jnp.where(allowed, scores_t, masked_fill)


def forward_kernel(heads_here, passes, tok, embed, gain, w_here, mixed, normed_out, qkv, lse, vt, ot):
    block = TOK_PASS
    full_len, width = tok.shape
    blocks = full_len // block
    count = passes[pl.program_id(0)]
    inverse = 1.0 / count.astype(F32)
    embed_rows = embed.shape[0]
    inner = heads_here * HEAD_DIM

    def project(index, carry):
        rows = pl.ds(pl.multiple_of(index * block, block), block)
        slot = lax.broadcasted_iota(jnp.int32, (block, embed_rows), 0) + index * block
        turn = jnp.floor((slot.astype(F32) + 0.5) * inverse).astype(jnp.int32)
        pass_index = slot - turn * count
        onehot = (pass_index == lax.broadcasted_iota(jnp.int32, (block, embed_rows), 1)).astype(F32)
        hidden = tok[rows, :].astype(F32) + matmul(onehot.astype(BF16), embed[...])
        normed = layer_norm(hidden, gain[...]).astype(BF16)
        normed_out[rows, :] = normed
        projected = matmul(normed, w_here[...])
        for piece in range(3 * heads_here):
            part = projected[:, piece * HEAD_DIM:(piece + 1) * HEAD_DIM]
            if piece < heads_here:
                part = part.astype(BF16).astype(F32) * HEAD_DIM ** (-0.5)
            qkv[piece, rows, :] = part.astype(BF16)
        vt[index] = projected[:, 2 * inner:].T.astype(BF16)
        return carry

    lax.fori_loop(0, blocks, project, 0)

    for at in range(blocks):
        here = slice(at * block, (at + 1) * block)

        @pl.when(at < count)
        def _():
            def one_head(head, carry):
                query = qkv[head, here, :]
                diagonal = causal(
                    lax.dot_general(qkv[heads_here + head, here, :], query, NT, preferred_element_type=F32), block
                )
                top = jnp.max(diagonal, axis=0, keepdims=True)
                if at:
                    before = lax.dot_general(
                        qkv[heads_here + head, 0:at * block, :], query, NT, preferred_element_type=F32
                    )
                    top = jnp.maximum(top, jnp.max(before, axis=0, keepdims=True))
                weight = jnp.exp(diagonal - top)
                total = jnp.sum(weight, axis=0, keepdims=True)
                head_rows = pl.ds(pl.multiple_of(head * HEAD_DIM, HEAD_DIM), HEAD_DIM)
                out = matmul(vt[at, head_rows, :], weight.astype(BF16))
                if at:
                    weight = jnp.exp(before - top)
                    total = total + jnp.sum(weight, axis=0, keepdims=True)
                    weight = weight.astype(BF16)
                    for key_at in range(at):
                        out = out + matmul(
                            vt[key_at, head_rows, :], weight[key_at * block:(key_at + 1) * block]
                        )
                ot[head_rows, :] = out * (1.0 / total)
                lse[pl.ds(head, 1), here] = top + jnp.log(total)
                return carry

            lax.fori_loop(0, heads_here, one_head, 0)
            mixed[here, :] = ot[...].T.astype(BF16)

        @pl.when(at >= count)
        def _():
            mixed[here, :] = jnp.zeros((block, inner), BF16)


def backward_kernel(heads_here, passes, qkv, lse, grad_mixed, grad_qkv, grad_heads, kt, sums, grads):
    block = TOK_PASS
    full_len = grad_mixed.shape[0]
    blocks = full_len // block
    count = passes[pl.program_id(0)]

    def split(index, carry):
        rows = pl.ds(pl.multiple_of(index * block, block), block)
        for head in range(heads_here):
            grad_heads[head, rows, :] = grad_mixed[rows, head * HEAD_DIM:(head + 1) * HEAD_DIM]
            kt[head, index] = qkv[heads_here + head, rows, :].astype(F32).T.astype(BF16)
        return carry

    lax.fori_loop(0, blocks, split, 0)

    def one_head(head, carry):
        sums[...] = jnp.zeros_like(sums)
        for at in range(blocks):
            here = slice(at * block, (at + 1) * block)

            @pl.when(at < count)
            def _():
                query = qkv[head, here, :]
                grad = grad_heads[head, here, :]
                row_lse = lse[pl.ds(head, 1), here]
                upto = (at + 1) * block
                keys = qkv[heads_here + head, 0:upto, :]
                values = qkv[2 * heads_here + head, 0:upto, :]
                scores = lax.dot_general(keys, query, NT, preferred_element_type=F32)
                pieces = [scores[:at * block]] if at else []
                pieces.append(causal(scores[at * block:], block))
                prob = [jnp.exp(piece - row_lse) for piece in pieces]
                back = lax.dot_general(values, grad, NT, preferred_element_type=F32)
                back = ([back[:at * block]] if at else []) + [back[at * block:]]
                inner = sum(
                    jnp.sum(one * two, axis=0, keepdims=True) for one, two in zip(prob, back)
                )
                bounds = ([(0, at * block)] if at else []) + [(at * block, upto)]
                turned = None
                for (low, high), one, two in zip(bounds, prob, back):
                    shift = (one * (two - inner)).astype(BF16)
                    sums[1, low:high, :] += matmul(one.astype(BF16), grad)
                    sums[0, low:high, :] += matmul(shift, query)
                    for key_at in range(low // block, high // block):
                        part = matmul(
                            kt[head, key_at], shift[key_at * block - low:(key_at + 1) * block - low]
                        )
                        turned = part if turned is None else turned + part
                grads[head, here, :] = (turned * HEAD_DIM ** (-0.5)).T.astype(BF16)

            @pl.when(at >= count)
            def _():
                grads[head, here, :] = jnp.zeros((block, HEAD_DIM), BF16)

        grads[heads_here + head] = sums[0].astype(BF16)
        grads[2 * heads_here + head] = sums[1].astype(BF16)
        return carry

    lax.fori_loop(0, heads_here, one_head, 0)

    def join(index, carry):
        rows = pl.ds(pl.multiple_of(index * block, block), block)
        grad_qkv[rows, :] = jnp.concatenate([grads[piece, rows, :] for piece in range(3 * heads_here)], axis=1)
        return carry

    lax.fori_loop(0, blocks, join, 0)


def attention_forward(tok_all, passes, embed, gain_one, w_here):
    items, full_len, width = tok_all.shape
    inner = w_here.shape[1] // 3
    heads_here = inner // HEAD_DIM
    blocks = full_len // TOK_PASS
    embed_low = jnp.zeros((128, width), BF16).at[:PASSES_MAX].set(embed)

    def whole(*dims):
        return pl.BlockSpec(dims, lambda i, *_: (0,) * len(dims))

    def per_item(*dims):
        return pl.BlockSpec((None, *dims), lambda i, *_: (i,) + (0,) * len(dims))

    return pl.pallas_call(
        lambda *refs: forward_kernel(heads_here, *refs),
        name="attention_forward",
        grid_spec=pltpu.PrefetchScalarGridSpec(
            num_scalar_prefetch=1,
            grid=(items,),
            in_specs=[per_item(full_len, width), whole(128, width), whole(1, width), whole(width, 3 * inner)],
            out_specs=[
                per_item(full_len, inner),
                per_item(full_len, width),
                per_item(3 * heads_here, full_len, HEAD_DIM),
                per_item(8, full_len),
            ],
            scratch_shapes=[
                pltpu.VMEM((blocks, inner, TOK_PASS), BF16),
                pltpu.VMEM((inner, TOK_PASS), F32),
            ],
        ),
        out_shape=[
            jax.ShapeDtypeStruct((items, full_len, inner), BF16),
            jax.ShapeDtypeStruct((items, full_len, width), BF16),
            jax.ShapeDtypeStruct((items, 3 * heads_here, full_len, HEAD_DIM), BF16),
            jax.ShapeDtypeStruct((items, 8, full_len), F32),
        ],
        compiler_params=pltpu.CompilerParams(vmem_limit_bytes=VMEM_LIMIT),
        cost_estimate=pl.CostEstimate(flops=8 * 10**9, bytes_accessed=16 * 10**6, transcendentals=6 * 10**6),
    )(passes, tok_all, embed_low, gain_one.astype(F32)[None], w_here)


def attention_backward(passes, qkv, lse, grad_mixed):
    items, full_len, inner = grad_mixed.shape
    heads_here = inner // HEAD_DIM
    blocks = full_len // TOK_PASS

    def per_item(*dims):
        return pl.BlockSpec((None, *dims), lambda i, *_: (i,) + (0,) * len(dims))

    return pl.pallas_call(
        lambda *refs: backward_kernel(heads_here, *refs),
        name="attention_backward",
        grid_spec=pltpu.PrefetchScalarGridSpec(
            num_scalar_prefetch=1,
            grid=(items,),
            in_specs=[
                per_item(3 * heads_here, full_len, HEAD_DIM),
                per_item(8, full_len),
                per_item(full_len, inner),
            ],
            out_specs=per_item(full_len, 3 * inner),
            scratch_shapes=[
                pltpu.VMEM((heads_here, full_len, HEAD_DIM), BF16),
                pltpu.VMEM((heads_here, blocks, HEAD_DIM, TOK_PASS), BF16),
                pltpu.VMEM((2, full_len, HEAD_DIM), F32),
                pltpu.VMEM((3 * heads_here, full_len, HEAD_DIM), BF16),
            ],
        ),
        out_shape=jax.ShapeDtypeStruct((items, full_len, 3 * inner), BF16),
        compiler_params=pltpu.CompilerParams(vmem_limit_bytes=VMEM_LIMIT),
        cost_estimate=pl.CostEstimate(flops=20 * 10**9, bytes_accessed=16 * 10**6, transcendentals=6 * 10**6),
    )(passes, qkv, lse, grad_mixed)


def reduce_rows(grad):
    low = grad.astype(BF16)
    return low


def on_device(tokens, passes, embed, gain_one, w_qkv, w_out, gain_two, w_up, w_down, cotangent):
    groups = lax.axis_size("heads")
    place = lax.axis_index("heads")
    item_count, span_here, width = tokens.shape
    row_count = item_count * span_here
    full_len = span_here * groups
    inner = width // groups
    slot_index = place * span_here + jnp.arange(span_here, dtype=jnp.int32)
    valid_len = TOK_PASS * passes
    row_mask = (slot_index[None, :] < valid_len[:, None]).astype(F32).reshape(row_count, 1)
    pass_index = (slot_index[None, :] % passes[:, None]).reshape(row_count, 1)
    onehot = (pass_index == jnp.arange(PASSES_MAX, dtype=jnp.int32)[None, :]).astype(BF16)

    tok_all = lax.all_gather(tokens, "heads", axis=1, tiled=True)
    w_here = lax.dynamic_index_in_dim(w_qkv.reshape(width, 3, groups, inner), place, 2, keepdims=False)
    w_here = w_here.reshape(width, 3 * inner)
    head_mixed, normed_all, qkv, lse = attention_forward(tok_all, passes, embed, gain_one, w_here)

    hidden = tokens.astype(F32).reshape(row_count, width) + matmul(onehot, embed)

    def to_slots(full):
        parts = full.reshape(item_count, groups, span_here, inner).transpose(1, 0, 2, 3)
        parts = lax.all_to_all(parts, "heads", split_axis=0, concat_axis=0, tiled=True)
        return parts.reshape(groups, row_count, inner)

    def to_heads(parts):
        parts = lax.all_to_all(
            parts.reshape(groups, item_count, span_here, inner), "heads", split_axis=0, concat_axis=0, tiled=True
        )
        return parts.transpose(1, 0, 2, 3).reshape(item_count, full_len, inner)

    mixed_rows = to_slots(head_mixed).transpose(1, 0, 2).reshape(row_count, width)
    middle = hidden + matmul(mixed_rows, w_out)
    second, norm_two_back = jax.vjp(layer_norm, middle, gain_two.astype(F32))
    second_low = second.astype(BF16)
    up_proj = matmul(second_low, w_up)
    active, gelu_back = jax.vjp(gelu_tanh, up_proj)
    active_low = active.astype(BF16)
    result = middle + matmul(active_low, w_down)
    outputs = (result * row_mask).astype(BF16).reshape(item_count, span_here, width)
    grad_result = cotangent.astype(F32).reshape(row_count, width) * row_mask
    grad_low = grad_result.astype(BF16)
    (grad_up,) = gelu_back(matmul(grad_low, w_down.T))
    grad_up_low = grad_up.astype(BF16)
    grad_middle_norm, grad_gain_two = norm_two_back(matmul(grad_up_low, w_up.T))
    grad_middle = grad_result + grad_middle_norm
    grad_branch = grad_middle.astype(BF16)
    grad_mixed = matmul(grad_branch, w_out.T).astype(BF16)
    head_grad = to_heads(grad_mixed.reshape(row_count, groups, inner).transpose(1, 0, 2))

    grad_w_down = matmul(active_low.T, grad_low).astype(BF16)
    grad_w_up = matmul(second_low.T, grad_up_low).astype(BF16)
    grad_w_out = matmul(mixed_rows.T, grad_branch).astype(BF16)

    def over_items(grad):
        return lax.psum_scatter(
            grad.reshape(groups, -1, *grad.shape[1:]), "items", scatter_dimension=1, tiled=True
        )

    head_grad, grad_w_down, grad_w_up, grad_w_out = lax.optimization_barrier(
        (head_grad, grad_w_down, grad_w_up, grad_w_out)
    )
    share_down = over_items(grad_w_down)
    share_up = over_items(grad_w_up)
    share_out = over_items(grad_w_out)

    grad_here = attention_backward(passes, qkv, lse, head_grad)
    flat_here = grad_here.reshape(item_count * full_len, 3 * inner)
    partial_norm = matmul(flat_here, w_here.T).astype(BF16).reshape(item_count, full_len, width)
    back_norm = lax.psum_scatter(partial_norm, "heads", scatter_dimension=1, tiled=True)
    grad_w_here = matmul(normed_all.reshape(item_count * full_len, width).T, flat_here).astype(BF16)
    share_qkv = over_items(grad_w_here)

    def finish(share):
        share = lax.psum_scatter(share, "heads", scatter_dimension=0, tiled=True)[0]
        return lax.all_gather(share, "items", axis=0, tiled=True).astype(F32)

    down_total, up_total, out_total = finish(share_down), finish(share_up), finish(share_out)
    share_qkv = lax.all_to_all(share_qkv, "heads", split_axis=0, concat_axis=0, tiled=True)
    qkv_total = lax.all_gather(share_qkv, "items", axis=1, tiled=True)
    qkv_total = qkv_total.reshape(groups, inner, 3, inner).transpose(1, 2, 0, 3).reshape(inner, 3 * width)
    qkv_total = qkv_total.astype(F32)

    _, norm_one_back = jax.vjp(layer_norm, hidden, gain_one.astype(F32))
    grad_hidden_norm, grad_gain_one = norm_one_back(back_norm.reshape(row_count, width).astype(F32))
    grad_hidden = grad_middle + grad_hidden_norm
    grad_tokens = grad_hidden.astype(BF16).reshape(item_count, span_here, width)
    grad_embed = lax.dot_general(
        onehot.astype(F32), grad_hidden, (((0,), (0,)), ((), ())), precision=lax.Precision.HIGHEST
    )
    small = jnp.concatenate([grad_embed, grad_gain_one[None], grad_gain_two[None]], axis=0)
    small = lax.psum(small, ("items", "heads"))
    small = lax.dynamic_slice_in_dim(small, place * inner, inner, axis=1)
    return (
        outputs,
        grad_tokens,
        small[:PASSES_MAX],
        small[PASSES_MAX],
        qkv_total,
        out_total,
        small[PASSES_MAX + 1],
        up_total,
        down_total,
    )


def solution(mesh):
    return jax.shard_map(
        on_device,
        mesh=mesh,
        in_specs=(
            P("items", "heads", None),
            P("items"),
            P(),
            P(),
            P(),
            P(),
            P(),
            P(),
            P(),
            P("items", "heads", None),
        ),
        out_specs=(
            P("items", "heads", None),
            P("items", "heads", None),
            P(None, "heads"),
            P("heads"),
            P("heads", None),
            P("heads", None),
            P("heads"),
            P("heads", None),
            P("heads", None),
        ),
        check_vma=False,
    )
```

```python
import jax
import jax.numpy as jnp
from jax import lax
from jax.experimental import pallas as pl
from jax.experimental.pallas import tpu as pltpu
from jax.sharding import PartitionSpec as P

HEADS = 12
HEAD_DIM = 64
PASSES_MAX = 5
TOK_PASS = 256

epsilon = 1e-05
masked_fill = -1e30
BF16 = jnp.bfloat16
F32 = jnp.float32
NT = (((1,), (1,)), ((), ()))
VMEM_LIMIT = 56 * 1024 * 1024


def matmul(left, right):
    return jnp.dot(left, right, preferred_element_type=F32)


def layer_norm(values_in, gain):
    centered = values_in - jnp.mean(values_in, axis=-1, keepdims=True)
    spread = jnp.mean(centered * centered, axis=-1, keepdims=True)
    return centered * lax.rsqrt(spread + epsilon) * gain


def gelu_tanh(values_in):
    return jax.nn.gelu(values_in, approximate=True)


def causal(scores_t, block):
    shape = (block, block)
    allowed = lax.broadcasted_iota(jnp.int32, shape, 0) <= lax.broadcasted_iota(jnp.int32, shape, 1)
    return jnp.where(allowed, scores_t, masked_fill)


def piece_rows(place, shift, groups, span):
    return pl.ds(pl.multiple_of(lax.rem(place + shift, groups) * span, span), span)


def forward_kernel(heads_here, groups, scalars, *refs):
    own, below, above = refs[0], refs[1:groups], refs[groups:2 * groups - 1]
    embed, gain, w_here = refs[2 * groups - 1:2 * groups + 2]
    pieces = refs[2 * groups + 2:3 * groups + 2]
    normed_out, qkv, lse, tok, vt, ot, mixed = refs[3 * groups + 2:]
    block = TOK_PASS
    full_len, width = tok.shape
    span = full_len // groups
    blocks = full_len // block
    place, count = scalars[0], scalars[1]
    inverse = 1.0 / count.astype(F32)
    embed_rows = embed.shape[0]
    inner = heads_here * HEAD_DIM

    tok[piece_rows(place, 0, groups, span), :] = own[...]
    for step in range(1, groups):

        @pl.when(place >= step)
        def _():
            tok[piece_rows(place, groups - step, groups, span), :] = below[step - 1][...]

        @pl.when(place + step < groups)
        def _():
            tok[piece_rows(place, step, groups, span), :] = above[step - 1][...]

    def project(index, carry):
        rows = pl.ds(pl.multiple_of(index * block, block), block)
        slot = lax.broadcasted_iota(jnp.int32, (block, embed_rows), 0) + index * block
        turn = jnp.floor((slot.astype(F32) + 0.5) * inverse).astype(jnp.int32)
        pass_index = slot - turn * count
        onehot = (pass_index == lax.broadcasted_iota(jnp.int32, (block, embed_rows), 1)).astype(F32)
        hidden = tok[rows, :].astype(F32) + matmul(onehot.astype(BF16), embed[...])
        normed = layer_norm(hidden, gain[...]).astype(BF16)
        normed_out[rows, :] = normed
        projected = matmul(normed, w_here[...])
        for piece in range(3 * heads_here):
            part = projected[:, piece * HEAD_DIM:(piece + 1) * HEAD_DIM]
            if piece < heads_here:
                part = part.astype(BF16).astype(F32) * HEAD_DIM ** (-0.5)
            qkv[piece, rows, :] = part.astype(BF16)
        vt[index] = projected[:, 2 * inner:].T.astype(BF16)
        return carry

    lax.fori_loop(0, blocks, project, 0)

    for at in range(blocks):
        here = slice(at * block, (at + 1) * block)

        @pl.when(at < count)
        def _():
            def one_head(head, carry):
                query = qkv[head, here, :]
                diagonal = causal(
                    lax.dot_general(qkv[heads_here + head, here, :], query, NT, preferred_element_type=F32), block
                )
                top = jnp.max(diagonal, axis=0, keepdims=True)
                if at:
                    before = lax.dot_general(
                        qkv[heads_here + head, 0:at * block, :], query, NT, preferred_element_type=F32
                    )
                    top = jnp.maximum(top, jnp.max(before, axis=0, keepdims=True))
                weight = jnp.exp(diagonal - top)
                total = jnp.sum(weight, axis=0, keepdims=True)
                head_rows = pl.ds(pl.multiple_of(head * HEAD_DIM, HEAD_DIM), HEAD_DIM)
                out = matmul(vt[at, head_rows, :], weight.astype(BF16))
                if at:
                    weight = jnp.exp(before - top)
                    total = total + jnp.sum(weight, axis=0, keepdims=True)
                    weight = weight.astype(BF16)
                    for key_at in range(at):
                        out = out + matmul(
                            vt[key_at, head_rows, :], weight[key_at * block:(key_at + 1) * block]
                        )
                ot[head_rows, :] = out * (1.0 / total)
                lse[pl.ds(head, 1), here] = top + jnp.log(total)
                return carry

            lax.fori_loop(0, heads_here, one_head, 0)
            mixed[here, :] = ot[...].T.astype(BF16)

        @pl.when(at >= count)
        def _():
            mixed[here, :] = jnp.zeros((block, inner), BF16)

    for shift in range(groups):
        pieces[shift][...] = mixed[piece_rows(place, shift, groups, span), :]


def backward_kernel(heads_here, groups, scalars, qkv, lse, *refs):
    grad_pieces, grad_qkv, outs = refs[:groups], refs[groups], refs[groups + 1:2 * groups + 1]
    grad_heads, kt, sums, grads = refs[2 * groups + 1:]
    block = TOK_PASS
    full_len = grad_qkv.shape[0]
    span = full_len // groups
    blocks = full_len // block
    place, count = scalars[0], scalars[1]

    for shift in range(groups):
        for head in range(heads_here):
            grad_heads[head, piece_rows(place, groups - shift, groups, span), :] = grad_pieces[shift][
                :, head * HEAD_DIM:(head + 1) * HEAD_DIM
            ]

    def split(index, carry):
        rows = pl.ds(pl.multiple_of(index * block, block), block)
        for head in range(heads_here):
            kt[head, index] = qkv[heads_here + head, rows, :].astype(F32).T.astype(BF16)
        return carry

    lax.fori_loop(0, blocks, split, 0)

    def one_head(head, carry):
        sums[...] = jnp.zeros_like(sums)
        for at in range(blocks):
            here = slice(at * block, (at + 1) * block)

            @pl.when(at < count)
            def _():
                query = qkv[head, here, :]
                grad = grad_heads[head, here, :]
                row_lse = lse[pl.ds(head, 1), here]
                upto = (at + 1) * block
                keys = qkv[heads_here + head, 0:upto, :]
                values = qkv[2 * heads_here + head, 0:upto, :]
                scores = lax.dot_general(keys, query, NT, preferred_element_type=F32)
                pieces = [scores[:at * block]] if at else []
                pieces.append(causal(scores[at * block:], block))
                prob = [jnp.exp(piece - row_lse) for piece in pieces]
                back = lax.dot_general(values, grad, NT, preferred_element_type=F32)
                back = ([back[:at * block]] if at else []) + [back[at * block:]]
                inner = sum(
                    jnp.sum(one * two, axis=0, keepdims=True) for one, two in zip(prob, back)
                )
                bounds = ([(0, at * block)] if at else []) + [(at * block, upto)]
                turned = None
                for (low, high), one, two in zip(bounds, prob, back):
                    shift = (one * (two - inner)).astype(BF16)
                    sums[1, low:high, :] += matmul(one.astype(BF16), grad)
                    sums[0, low:high, :] += matmul(shift, query)
                    for key_at in range(low // block, high // block):
                        part = matmul(
                            kt[head, key_at], shift[key_at * block - low:(key_at + 1) * block - low]
                        )
                        turned = part if turned is None else turned + part
                grads[head, here, :] = (turned * HEAD_DIM ** (-0.5)).T.astype(BF16)

            @pl.when(at >= count)
            def _():
                grads[head, here, :] = jnp.zeros((block, HEAD_DIM), BF16)

        grads[heads_here + head] = sums[0].astype(BF16)
        grads[2 * heads_here + head] = sums[1].astype(BF16)
        return carry

    lax.fori_loop(0, heads_here, one_head, 0)

    def join(index, carry):
        rows = pl.ds(pl.multiple_of(index * block, block), block)
        grad_qkv[rows, :] = jnp.concatenate([grads[piece, rows, :] for piece in range(3 * heads_here)], axis=1)
        return carry

    lax.fori_loop(0, blocks, join, 0)

    for shift in range(groups):
        outs[shift][...] = grad_qkv[piece_rows(place, shift, groups, span), :]


def attention_forward(scalars, own, below, above, embed_low, gain_one, w_here):
    groups = len(below) + 1
    span, width = own.shape
    full_len = span * groups
    inner = w_here.shape[1] // 3
    heads_here = inner // HEAD_DIM
    blocks = full_len // TOK_PASS
    vmem = pl.BlockSpec(memory_space=pltpu.VMEM)
    outs = pl.pallas_call(
        lambda *refs: forward_kernel(heads_here, groups, *refs),
        name="attention_forward",
        in_specs=[pl.BlockSpec(memory_space=pltpu.SMEM)] + [vmem] * (2 * groups + 2),
        out_specs=[vmem] * (groups + 3),
        scratch_shapes=[
            pltpu.VMEM((full_len, width), BF16),
            pltpu.VMEM((blocks, inner, TOK_PASS), BF16),
            pltpu.VMEM((inner, TOK_PASS), F32),
            pltpu.VMEM((full_len, inner), BF16),
        ],
        out_shape=[jax.ShapeDtypeStruct((span, inner), BF16)] * groups
        + [
            jax.ShapeDtypeStruct((full_len, width), BF16),
            jax.ShapeDtypeStruct((3 * heads_here, full_len, HEAD_DIM), BF16),
            jax.ShapeDtypeStruct((8, full_len), F32),
        ],
        compiler_params=pltpu.CompilerParams(vmem_limit_bytes=VMEM_LIMIT),
        cost_estimate=pl.CostEstimate(flops=9 * 10**9, bytes_accessed=12 * 10**6, transcendentals=3 * 10**6),
    )(scalars, own, *below, *above, embed_low, gain_one, w_here)
    return outs[:groups], outs[groups], outs[groups + 1], outs[groups + 2]


def attention_backward(scalars, qkv, lse, grad_pieces):
    groups = len(grad_pieces)
    span, inner = grad_pieces[0].shape
    full_len = span * groups
    heads_here = inner // HEAD_DIM
    blocks = full_len // TOK_PASS
    vmem = pl.BlockSpec(memory_space=pltpu.VMEM)
    outs = pl.pallas_call(
        lambda *refs: backward_kernel(heads_here, groups, *refs),
        name="attention_backward",
        in_specs=[pl.BlockSpec(memory_space=pltpu.SMEM)] + [vmem] * (groups + 2),
        out_specs=[vmem] * (groups + 1),
        scratch_shapes=[
            pltpu.VMEM((heads_here, full_len, HEAD_DIM), BF16),
            pltpu.VMEM((heads_here, blocks, HEAD_DIM, TOK_PASS), BF16),
            pltpu.VMEM((2, full_len, HEAD_DIM), F32),
            pltpu.VMEM((3 * heads_here, full_len, HEAD_DIM), BF16),
        ],
        out_shape=[jax.ShapeDtypeStruct((full_len, 3 * inner), BF16)]
        + [jax.ShapeDtypeStruct((span, 3 * inner), BF16)] * groups,
        compiler_params=pltpu.CompilerParams(vmem_limit_bytes=VMEM_LIMIT),
        cost_estimate=pl.CostEstimate(flops=9 * 10**9, bytes_accessed=8 * 10**6, transcendentals=3 * 10**6),
    )(scalars, qkv, lse, *grad_pieces)
    return outs[0], outs[1:]


def shift_heads(piece, shift, groups):
    return lax.ppermute(piece, "heads", [(at, (at + shift) % groups) for at in range(groups)])


def swap_items(piece, bit):
    size = lax.axis_size("items")
    return lax.ppermute(piece, "items", [(at, at ^ (1 << bit)) for at in range(size)])


def item_bit(bit):
    return (lax.axis_index("items") >> bit) & 1


def sum_items(grad, axis, order):
    for bit in order:
        half = grad.shape[axis] // 2
        mine = item_bit(bit)
        sent = lax.dynamic_slice_in_dim(grad, (1 - mine) * half, half, axis)
        kept = lax.dynamic_slice_in_dim(grad, mine * half, half, axis)
        grad = (kept.astype(F32) + swap_items(sent, bit).astype(F32)).astype(BF16)
    return grad


def gather_items(part, axis, order):
    for bit in reversed(order):
        other = swap_items(part, bit)
        high = item_bit(bit) == 1
        part = jnp.concatenate([jnp.where(high, other, part), jnp.where(high, part, other)], axis=axis)
    return part


def scatter_heads(grad, groups, static_order):
    place = lax.axis_index("heads")

    def part_for(shift):
        if static_order:
            return grad[(groups - shift) % groups]
        return lax.dynamic_index_in_dim(grad, (place + shift) % groups, 0, keepdims=False)

    return [part_for(0)] + [shift_heads(part_for(shift), shift, groups) for shift in range(1, groups)]


def total_of(parts):
    total = parts[0].astype(F32)
    for part in parts[1:]:
        total = total + part.astype(F32)
    return total


def on_device(tokens, passes, embed, gain_one, w_qkv, w_out, gain_two, w_up, w_down, cotangent):
    groups = lax.axis_size("heads")
    place = lax.axis_index("heads")
    item_count, span_here, width = tokens.shape
    row_count = item_count * span_here
    inner = width // groups
    bits = lax.axis_size("items").bit_length() - 1
    order_a = list(range(bits))
    order_b = [0] + list(range(bits - 1, 0, -1))

    belows, aboves = [], []
    for item in range(item_count):
        below, above = [], []
        low = high = tokens[item]
        for step in range(1, groups):
            low = lax.ppermute(low, "heads", [(at, at + 1) for at in range(step - 1, groups - 1)])
            high = lax.ppermute(high, "heads", [(at, at - 1) for at in range(1, groups - step + 1)])
            below.append(low)
            above.append(high)
        belows.append(below)
        aboves.append(above)

    slot_index = place * span_here + jnp.arange(span_here, dtype=jnp.int32)
    valid_len = TOK_PASS * passes
    row_mask = (slot_index[None, :] < valid_len[:, None]).astype(F32).reshape(row_count, 1)
    pass_index = (slot_index[None, :] % passes[:, None]).reshape(row_count, 1)
    onehot = (pass_index == jnp.arange(PASSES_MAX, dtype=jnp.int32)[None, :]).astype(BF16)
    w_grouped = w_qkv.reshape(width, 3, groups, inner)

    def columns_of(shift):
        piece = lax.dynamic_index_in_dim(w_grouped, (place - shift) % groups, 2, keepdims=False)
        return piece.reshape(width, 3 * inner)

    w_shifted = [columns_of(shift) for shift in range(groups)]
    out_shifted = [
        lax.dynamic_slice_in_dim(w_out, ((place - shift) % groups) * inner, inner, 0) for shift in range(groups)
    ]
    hidden = tokens.astype(F32).reshape(row_count, width) + matmul(onehot, embed)
    grad_result = cotangent.astype(F32).reshape(row_count, width) * row_mask
    grad_low = grad_result.astype(BF16)
    grad_active = matmul(grad_low, w_down.T).astype(BF16)
    embed_low = jnp.zeros((128, width), BF16).at[:PASSES_MAX].set(embed)
    gain_row = gain_one.astype(F32)[None]

    kept, mixed_parts = [], []
    for item in range(item_count):
        scalars = jnp.stack([place, passes[item]]).astype(jnp.int32)
        pieces, normed_all, qkv, lse = attention_forward(
            scalars, tokens[item], belows[item], aboves[item], embed_low, gain_row, w_shifted[0]
        )
        kept.append((scalars, normed_all, qkv, lse))
        mixed_parts.append(
            jnp.concatenate([pieces[0]] + [shift_heads(pieces[s], s, groups) for s in range(1, groups)], axis=1)
        )

    mixed_rows = jnp.concatenate(mixed_parts, axis=0)
    middle = hidden + matmul(mixed_rows, jnp.concatenate(out_shifted, axis=0))
    second, norm_two_back = jax.vjp(layer_norm, middle, gain_two.astype(F32))
    second_low = second.astype(BF16)
    up_proj = matmul(second_low, w_up)
    active, gelu_back = jax.vjp(gelu_tanh, up_proj)
    active_low = active.astype(BF16)
    (grad_up,) = gelu_back(grad_active.astype(F32))
    grad_up_low = grad_up.astype(BF16)
    grad_middle_norm, grad_gain_two = norm_two_back(matmul(grad_up_low, w_up.T))
    grad_middle = grad_result + grad_middle_norm
    grad_branch = grad_middle.astype(BF16)
    grad_pieces = [
        matmul(grad_branch, out_shifted[(groups - shift) % groups].T).astype(BF16) for shift in range(groups)
    ]
    grad_pieces = [grad_pieces[0]] + [
        shift_heads(grad_pieces[shift], shift, groups) for shift in range(1, groups)
    ]

    grad_w_down = matmul(active_low.T, grad_low).astype(BF16)
    grad_w_up = matmul(second_low.T, grad_up_low).astype(BF16)
    grad_w_out = matmul(mixed_rows.T, grad_branch).astype(BF16)
    grad_pieces, grad_w_down, grad_w_up = lax.optimization_barrier((grad_pieces, grad_w_down, grad_w_up))
    share_down = sum_items(grad_w_down.reshape(groups, -1, width), 1, order_a)
    share_up = sum_items(grad_w_up.reshape(groups, inner, -1), 2, order_b)
    result = middle + matmul(active_low, w_down)
    outputs = (result * row_mask).astype(BF16).reshape(item_count, span_here, width)

    flat_here, arrived = [], []
    for item in range(item_count):
        scalars, _, qkv, lse = kept[item]
        whole, pieces = attention_backward(
            scalars, qkv, lse, [piece[item * span_here:(item + 1) * span_here] for piece in grad_pieces]
        )
        flat_here.append(whole)
        arrived.append([pieces[0]] + [shift_heads(pieces[s], s, groups) for s in range(1, groups)])

    normed_rows = jnp.concatenate([entry[1] for entry in kept], axis=0)
    grad_w_here = matmul(normed_rows.T, jnp.concatenate(flat_here, axis=0)).astype(BF16)

    down_total = gather_items(total_of(scatter_heads(share_down, groups, False)).astype(BF16), 0, order_a)
    up_total = gather_items(total_of(scatter_heads(share_up, groups, False)).astype(BF16), 1, order_b)

    qkv_rows = jnp.concatenate([lax.dynamic_slice_in_dim(
        grad_w_here, ((place - shift) % groups) * inner, inner, 0) for shift in range(groups)], axis=0)
    late = jnp.concatenate([grad_w_out, qkv_rows], axis=1).reshape(groups, 1 << bits, -1, width + 3 * inner)
    late = sum_items(late, 1, order_b)[:, 0]
    late = scatter_heads(late, groups, True)
    out_part = total_of([part[:, :width] for part in late]).astype(BF16)
    late = jnp.concatenate([out_part] + [part[:, width:] for part in late], axis=1)[None]
    late = gather_items(late, 0, order_b).reshape(inner, -1)
    out_total = late[:, :width]
    by_shift = late[:, width:].reshape(inner, groups, 3, inner)
    qkv_total = jnp.stack(
        [lax.dynamic_index_in_dim(by_shift, (place - group) % groups, 1, keepdims=False) for group in range(groups)],
        axis=2,
    ).reshape(inner, 3 * width)

    back_rows = jnp.concatenate([jnp.concatenate(parts, axis=1) for parts in arrived], axis=0)
    back_norm = matmul(back_rows, jnp.concatenate(w_shifted, axis=1).T)
    _, norm_one_back = jax.vjp(layer_norm, hidden, gain_one.astype(F32))
    grad_hidden_norm, grad_gain_one = norm_one_back(back_norm)
    grad_hidden = grad_middle + grad_hidden_norm
    grad_tokens = grad_hidden.astype(BF16).reshape(item_count, span_here, width)
    grad_embed = lax.dot_general(
        onehot.astype(F32), grad_hidden, (((0,), (0,)), ((), ())), precision=lax.Precision.HIGHEST
    )
    small = jnp.concatenate([grad_embed, grad_gain_one[None], grad_gain_two[None]], axis=0)
    small = total_of(scatter_heads(small.reshape(-1, groups, inner).transpose(1, 0, 2), groups, False))
    for bit in range(bits):
        small = small + swap_items(small, bit)
    return (
        outputs,
        grad_tokens,
        small[:PASSES_MAX],
        small[PASSES_MAX],
        qkv_total.astype(F32),
        out_total.astype(F32),
        small[PASSES_MAX + 1],
        up_total.astype(F32),
        down_total.astype(F32),
    )


def solution(mesh):
    return jax.shard_map(
        on_device,
        mesh=mesh,
        in_specs=(
            P("items", "heads", None),
            P("items"),
            P(),
            P(),
            P(),
            P(),
            P(),
            P(),
            P(),
            P("items", "heads", None),
        ),
        out_specs=(
            P("items", "heads", None),
            P("items", "heads", None),
            P(None, "heads"),
            P("heads"),
            P("heads", None),
            P("heads", None),
            P("heads"),
            P("heads", None),
            P("heads", None),
        ),
        check_vma=False,
    )
```

```python
import jax
import jax.numpy as jnp
from jax import lax
from jax.experimental import pallas as pl
from jax.experimental.pallas import tpu as pltpu
from jax.sharding import PartitionSpec as P


HEAD_DIM = 64
PASSES_MAX = 5
TOK_PASS = 256

epsilon = 1e-05
masked_fill = -1e30
BF16 = jnp.bfloat16
F32 = jnp.float32
NT = (((1,), (1,)), ((), ()))
VMEM_LIMIT = 56 * 1024 * 1024


def matmul(left, right):
    return jnp.dot(left, right, preferred_element_type=F32)


def layer_norm(values_in, gain):
    centered = values_in - jnp.mean(values_in, axis=-1, keepdims=True)
    spread = jnp.mean(centered * centered, axis=-1, keepdims=True)
    return centered * lax.rsqrt(spread + epsilon) * gain


def gelu_tanh(values_in):
    return jax.nn.gelu(values_in, approximate=True)


def causal(scores_t, block):
    shape = (block, block)
    allowed = lax.broadcasted_iota(jnp.int32, shape, 0) <= lax.broadcasted_iota(jnp.int32, shape, 1)
    return jnp.where(allowed, scores_t, masked_fill)


def piece_rows(place, shift, groups, span):
    return pl.ds(pl.multiple_of(lax.rem(place + shift, groups) * span, span), span)


def forward_kernel(heads_here, groups, scalars, *refs):
    own, below, above = refs[0], refs[1:groups], refs[groups:2 * groups - 1]
    embed, gain, w_here = refs[2 * groups - 1:2 * groups + 2]
    pieces = refs[2 * groups + 2:3 * groups + 2]
    normed_out, qkv, lse, tok, vt, ot, mixed = refs[3 * groups + 2:]
    block = TOK_PASS
    full_len, _ = tok.shape
    span = full_len // groups
    blocks = full_len // block
    place, count = scalars[0], scalars[1]
    inverse = 1.0 / count.astype(F32)
    embed_rows = embed.shape[0]
    inner = heads_here * HEAD_DIM

    tok[piece_rows(place, 0, groups, span), :] = own[...]
    for step in range(1, groups):

        @pl.when(place >= step)
        def _():
            tok[piece_rows(place, groups - step, groups, span), :] = below[step - 1][...]

        @pl.when(place + step < groups)
        def _():
            tok[piece_rows(place, step, groups, span), :] = above[step - 1][...]

    def project(index, carry):
        rows = pl.ds(pl.multiple_of(index * block, block), block)
        slot = lax.broadcasted_iota(jnp.int32, (block, embed_rows), 0) + index * block
        turn = jnp.floor((slot.astype(F32) + 0.5) * inverse).astype(jnp.int32)
        pass_index = slot - turn * count
        onehot = (pass_index == lax.broadcasted_iota(jnp.int32, (block, embed_rows), 1)).astype(F32)
        hidden = tok[rows, :].astype(F32) + matmul(onehot.astype(BF16), embed[...])
        normed = layer_norm(hidden, gain[...]).astype(BF16)
        normed_out[rows, :] = normed
        projected = matmul(normed, w_here[...])
        for piece in range(3 * heads_here):
            part = projected[:, piece * HEAD_DIM:(piece + 1) * HEAD_DIM]
            if piece < heads_here:
                part = part.astype(BF16).astype(F32) * HEAD_DIM ** (-0.5)
            qkv[piece, rows, :] = part.astype(BF16)
        vt[index] = projected[:, 2 * inner:].T.astype(BF16)
        return carry

    lax.fori_loop(0, blocks, project, 0)

    for at in range(blocks):
        here = slice(at * block, (at + 1) * block)

        @pl.when(at < count)
        def _():
            def one_head(head, carry):
                query = qkv[head, here, :]
                diagonal = causal(
                    lax.dot_general(qkv[heads_here + head, here, :], query, NT, preferred_element_type=F32), block
                )
                top = jnp.max(diagonal, axis=0, keepdims=True)
                if at:
                    before = lax.dot_general(
                        qkv[heads_here + head, 0:at * block, :], query, NT, preferred_element_type=F32
                    )
                    top = jnp.maximum(top, jnp.max(before, axis=0, keepdims=True))
                weight = jnp.exp(diagonal - top)
                total = jnp.sum(weight, axis=0, keepdims=True)
                head_rows = pl.ds(pl.multiple_of(head * HEAD_DIM, HEAD_DIM), HEAD_DIM)
                out = matmul(vt[at, head_rows, :], weight.astype(BF16))
                if at:
                    weight = jnp.exp(before - top)
                    total = total + jnp.sum(weight, axis=0, keepdims=True)
                    weight = weight.astype(BF16)
                    for key_at in range(at):
                        out = out + matmul(
                            vt[key_at, head_rows, :], weight[key_at * block:(key_at + 1) * block]
                        )
                ot[head_rows, :] = out * (1.0 / total)
                lse[pl.ds(head, 1), here] = top + jnp.log(total)
                return carry

            lax.fori_loop(0, heads_here, one_head, 0)
            mixed[here, :] = ot[...].T.astype(BF16)

        @pl.when(at >= count)
        def _():
            mixed[here, :] = jnp.zeros((block, inner), BF16)

    for shift in range(groups):
        pieces[shift][...] = mixed[piece_rows(place, shift, groups, span), :]


def backward_kernel(heads_here, groups, scalars, qkv, lse, *refs):
    grad_pieces, grad_qkv, outs = refs[:groups], refs[groups], refs[groups + 1:2 * groups + 1]
    grad_heads, kt, sums, grads = refs[2 * groups + 1:]
    block = TOK_PASS
    full_len = grad_qkv.shape[0]
    span = full_len // groups
    blocks = full_len // block
    place, count = scalars[0], scalars[1]

    for shift in range(groups):
        for head in range(heads_here):
            grad_heads[head, piece_rows(place, groups - shift, groups, span), :] = grad_pieces[shift][
                :, head * HEAD_DIM:(head + 1) * HEAD_DIM
            ]

    def split(index, carry):
        rows = pl.ds(pl.multiple_of(index * block, block), block)
        for head in range(heads_here):
            kt[head, index] = qkv[heads_here + head, rows, :].astype(F32).T.astype(BF16)
        return carry

    lax.fori_loop(0, blocks, split, 0)

    def one_head(head, carry):
        sums[...] = jnp.zeros_like(sums)
        for at in range(blocks):
            here = slice(at * block, (at + 1) * block)

            @pl.when(at < count)
            def _():
                query = qkv[head, here, :]
                grad = grad_heads[head, here, :]
                row_lse = lse[pl.ds(head, 1), here]
                upto = (at + 1) * block
                keys = qkv[heads_here + head, 0:upto, :]
                values = qkv[2 * heads_here + head, 0:upto, :]
                scores = lax.dot_general(keys, query, NT, preferred_element_type=F32)
                pieces = [scores[:at * block]] if at else []
                pieces.append(causal(scores[at * block:], block))
                prob = [jnp.exp(piece - row_lse) for piece in pieces]
                back = lax.dot_general(values, grad, NT, preferred_element_type=F32)
                back = ([back[:at * block]] if at else []) + [back[at * block:]]
                inner = sum(
                    jnp.sum(one * two, axis=0, keepdims=True) for one, two in zip(prob, back)
                )
                bounds = ([(0, at * block)] if at else []) + [(at * block, upto)]
                turned = None
                for (low, high), one, two in zip(bounds, prob, back):
                    shift = (one * (two - inner)).astype(BF16)
                    sums[1, low:high, :] += matmul(one.astype(BF16), grad)
                    sums[0, low:high, :] += matmul(shift, query)
                    for key_at in range(low // block, high // block):
                        part = matmul(
                            kt[head, key_at], shift[key_at * block - low:(key_at + 1) * block - low]
                        )
                        turned = part if turned is None else turned + part
                grads[head, here, :] = (turned * HEAD_DIM ** (-0.5)).T.astype(BF16)

            @pl.when(at >= count)
            def _():
                grads[head, here, :] = jnp.zeros((block, HEAD_DIM), BF16)

        grads[heads_here + head] = sums[0].astype(BF16)
        grads[2 * heads_here + head] = sums[1].astype(BF16)
        return carry

    lax.fori_loop(0, heads_here, one_head, 0)

    def join(index, carry):
        rows = pl.ds(pl.multiple_of(index * block, block), block)
        grad_qkv[rows, :] = jnp.concatenate([grads[piece, rows, :] for piece in range(3 * heads_here)], axis=1)
        return carry

    lax.fori_loop(0, blocks, join, 0)

    for shift in range(groups):
        outs[shift][...] = grad_qkv[piece_rows(place, shift, groups, span), :]


def attention_forward(scalars, own, below, above, embed_low, gain_one, w_here):
    groups = len(below) + 1
    span, width = own.shape
    full_len = span * groups
    inner = w_here.shape[1] // 3
    heads_here = inner // HEAD_DIM
    blocks = full_len // TOK_PASS
    vmem = pl.BlockSpec(memory_space=pltpu.VMEM)
    outs = pl.pallas_call(
        lambda *refs: forward_kernel(heads_here, groups, *refs),
        name="attention_forward",
        in_specs=[pl.BlockSpec(memory_space=pltpu.SMEM)] + [vmem] * (2 * groups + 2),
        out_specs=[vmem] * (groups + 3),
        scratch_shapes=[
            pltpu.VMEM((full_len, width), BF16),
            pltpu.VMEM((blocks, inner, TOK_PASS), BF16),
            pltpu.VMEM((inner, TOK_PASS), F32),
            pltpu.VMEM((full_len, inner), BF16),
        ],
        out_shape=[jax.ShapeDtypeStruct((span, inner), BF16)] * groups
        + [
            jax.ShapeDtypeStruct((full_len, width), BF16),
            jax.ShapeDtypeStruct((3 * heads_here, full_len, HEAD_DIM), BF16),
            jax.ShapeDtypeStruct((8, full_len), F32),
        ],
        compiler_params=pltpu.CompilerParams(vmem_limit_bytes=VMEM_LIMIT),
        cost_estimate=pl.CostEstimate(flops=9 * 10**9, bytes_accessed=12 * 10**6, transcendentals=3 * 10**6),
    )(scalars, own, *below, *above, embed_low, gain_one, w_here)
    return outs[:groups], outs[groups], outs[groups + 1], outs[groups + 2]


def attention_backward(scalars, qkv, lse, grad_pieces):
    groups = len(grad_pieces)
    span, inner = grad_pieces[0].shape
    full_len = span * groups
    heads_here = inner // HEAD_DIM
    blocks = full_len // TOK_PASS
    vmem = pl.BlockSpec(memory_space=pltpu.VMEM)
    outs = pl.pallas_call(
        lambda *refs: backward_kernel(heads_here, groups, *refs),
        name="attention_backward",
        in_specs=[pl.BlockSpec(memory_space=pltpu.SMEM)] + [vmem] * (groups + 2),
        out_specs=[vmem] * (groups + 1),
        scratch_shapes=[
            pltpu.VMEM((heads_here, full_len, HEAD_DIM), BF16),
            pltpu.VMEM((heads_here, blocks, HEAD_DIM, TOK_PASS), BF16),
            pltpu.VMEM((2, full_len, HEAD_DIM), F32),
            pltpu.VMEM((3 * heads_here, full_len, HEAD_DIM), BF16),
        ],
        out_shape=[jax.ShapeDtypeStruct((full_len, 3 * inner), BF16)]
        + [jax.ShapeDtypeStruct((span, 3 * inner), BF16)] * groups,
        compiler_params=pltpu.CompilerParams(vmem_limit_bytes=VMEM_LIMIT),
        cost_estimate=pl.CostEstimate(flops=9 * 10**9, bytes_accessed=8 * 10**6, transcendentals=3 * 10**6),
    )(scalars, qkv, lse, *grad_pieces)
    return outs[0], outs[1:]


def shift_heads(piece, shift, groups):
    return lax.ppermute(piece, "heads", [(at, (at + shift) % groups) for at in range(groups)])


def swap_items(piece, bit):
    size = lax.axis_size("items")
    return lax.ppermute(piece, "items", [(at, at ^ (1 << bit)) for at in range(size)])


def item_bit(bit):
    return (lax.axis_index("items") >> bit) & 1


def halve(grad, axis, bit):
    half = grad.shape[axis] // 2
    mine = item_bit(bit)
    sent = lax.dynamic_slice_in_dim(grad, (1 - mine) * half, half, axis)
    kept = lax.dynamic_slice_in_dim(grad, mine * half, half, axis)
    return (kept.astype(F32) + swap_items(sent, bit).astype(F32)).astype(BF16)


def sum_items(grad, axis, order):
    for bit in order:
        grad = halve(grad, axis, bit)
    return grad


def gather_items(part, axis, order):
    for bit in reversed(order):
        other = swap_items(part, bit)
        high = item_bit(bit) == 1
        part = jnp.concatenate([jnp.where(high, other, part), jnp.where(high, part, other)], axis=axis)
    return part


def scatter_heads(grad, groups, static_order):
    place = lax.axis_index("heads")

    def part_for(shift):
        if static_order:
            return grad[(groups - shift) % groups]
        return lax.dynamic_index_in_dim(grad, (place + shift) % groups, 0, keepdims=False)

    return [part_for(0)] + [shift_heads(part_for(shift), shift, groups) for shift in range(1, groups)]


def total_of(parts):
    total = parts[0].astype(F32)
    for part in parts[1:]:
        total = total + part.astype(F32)
    return total


def layer(tokens, passes, embed, gain_one, w_qkv, w_out, gain_two, w_up, w_down, cotangent):
    groups = lax.axis_size("heads")
    place = lax.axis_index("heads")
    item_count, span_here, width = tokens.shape
    row_count = item_count * span_here
    inner = width // groups
    bits = lax.axis_size("items").bit_length() - 1
    order_a = list(range(bits))
    order_b = [0] + list(range(bits - 1, 0, -1))

    belows, aboves = [], []
    for item in range(item_count):
        below, above = [], []
        low = high = tokens[item]
        if item:
            low, high, *_ = lax.optimization_barrier((low, high, belows[-1][:2], aboves[-1][:2]))
        for step in range(1, groups):
            low = lax.ppermute(low, "heads", [(at, at + 1) for at in range(step - 1, groups - 1)])
            high = lax.ppermute(high, "heads", [(at, at - 1) for at in range(1, groups - step + 1)])
            below.append(low)
            above.append(high)
        belows.append(below)
        aboves.append(above)

    slot_index = place * span_here + jnp.arange(span_here, dtype=jnp.int32)
    valid_len = TOK_PASS * passes
    row_mask = (slot_index[None, :] < valid_len[:, None]).astype(F32).reshape(row_count, 1)
    pass_index = (slot_index[None, :] % passes[:, None]).reshape(row_count, 1)
    onehot = (pass_index == jnp.arange(PASSES_MAX, dtype=jnp.int32)[None, :]).astype(BF16)
    w_grouped = w_qkv.reshape(width, 3, groups, inner)

    def columns_of(shift):
        piece = lax.dynamic_index_in_dim(w_grouped, (place - shift) % groups, 2, keepdims=False)
        return piece.reshape(width, 3 * inner)

    w_shifted = [columns_of(shift) for shift in range(groups)]
    out_shifted = [
        lax.dynamic_slice_in_dim(w_out, ((place - shift) % groups) * inner, inner, 0) for shift in range(groups)
    ]
    hidden = tokens.astype(F32).reshape(row_count, width) + matmul(onehot, embed)
    grad_result = cotangent.astype(F32).reshape(row_count, width) * row_mask
    grad_low = grad_result.astype(BF16)
    grad_active = matmul(grad_low, w_down.T).astype(BF16)
    embed_low = jnp.zeros((128, width), BF16).at[:PASSES_MAX].set(embed)
    gain_row = gain_one.astype(F32)[None]

    kept, mixed_parts = [], []
    for item in range(item_count):
        scalars = jnp.stack([place, passes[item]]).astype(jnp.int32)
        pieces, normed_all, qkv, lse = attention_forward(
            scalars, tokens[item], belows[item], aboves[item], embed_low, gain_row, w_shifted[0]
        )
        kept.append((scalars, normed_all, qkv, lse))
        mixed_parts.append(
            jnp.concatenate([pieces[0]] + [shift_heads(pieces[s], s, groups) for s in range(1, groups)], axis=1)
        )

    mixed_rows = jnp.concatenate(mixed_parts, axis=0)
    middle = hidden + matmul(mixed_rows, jnp.concatenate(out_shifted, axis=0))
    second, norm_two_back = jax.vjp(layer_norm, middle, gain_two.astype(F32))
    second_low = second.astype(BF16)
    up_proj = matmul(second_low, w_up)
    active, gelu_back = jax.vjp(gelu_tanh, up_proj)
    active_low = active.astype(BF16)
    (grad_up,) = gelu_back(grad_active.astype(F32))
    grad_up_low = grad_up.astype(BF16)
    grad_middle_norm, grad_gain_two = norm_two_back(matmul(grad_up_low, w_up.T))
    grad_middle = grad_result + grad_middle_norm
    grad_branch = grad_middle.astype(BF16)
    grad_pieces = [
        matmul(grad_branch, out_shifted[(groups - shift) % groups].T).astype(BF16) for shift in range(groups)
    ]
    grad_pieces, active_low, second_low = lax.optimization_barrier((grad_pieces, active_low, second_low))
    for shift in range(1, groups):
        grad_pieces[shift] = shift_heads(grad_pieces[shift], shift, groups)

    grad_w_down = matmul(active_low.T, grad_low).astype(BF16)
    grad_w_up = matmul(second_low.T, grad_up_low).astype(BF16)
    grad_w_out = matmul(mixed_rows.T, grad_branch).astype(BF16)
    share_down = halve(grad_w_down.reshape(groups, -1, width), 1, order_a[0])
    share_up = halve(grad_w_up.reshape(groups, inner, -1), 2, order_b[0])
    result = middle + matmul(active_low, w_down)
    outputs = (result * row_mask).astype(BF16).reshape(item_count, span_here, width)

    grad_pieces, share_down, share_up, outputs = lax.optimization_barrier(
        (grad_pieces, share_down, share_up, outputs)
    )
    share_down = halve(share_down, 1, order_a[1])
    share_up = halve(share_up, 2, order_b[1])

    flat_here, arrived = [], []
    for item in range(item_count):
        scalars, _, qkv, lse = kept[item]
        whole, pieces = attention_backward(
            scalars, qkv, lse, [piece[item * span_here:(item + 1) * span_here] for piece in grad_pieces]
        )
        flat_here.append(whole)
        parts = [pieces[0]]
        for shift in range(1, groups):
            parts.append(shift_heads(pieces[shift], shift, groups))
        arrived.append(parts)

    flat_here, share_down, share_up = lax.optimization_barrier((flat_here, share_down, share_up))
    share_down = sum_items(share_down, 1, order_a[2:])
    share_up = sum_items(share_up, 2, order_b[2:])
    grad_w_here = total_of(
        [matmul(entry[1].T, whole) for entry, whole in zip(kept, flat_here)]
    ).astype(BF16)
    grad_w_here, share_down, share_up = lax.optimization_barrier((grad_w_here, share_down, share_up))
    share_down = total_of(scatter_heads(share_down, groups, False)).astype(BF16)
    share_up = total_of(scatter_heads(share_up, groups, False)).astype(BF16)

    qkv_rows = jnp.concatenate([lax.dynamic_slice_in_dim(
        grad_w_here, ((place - shift) % groups) * inner, inner, 0) for shift in range(groups)], axis=0)
    late = jnp.concatenate([grad_w_out, qkv_rows], axis=1).reshape(groups, 1 << bits, -1, width + 3 * inner)
    late = sum_items(late, 1, order_b)[:, 0]
    arrived, share_down, share_up, late = lax.optimization_barrier((arrived, share_down, share_up, late))
    down_total = gather_items(share_down, 0, order_a)
    up_total = gather_items(share_up, 1, order_b)
    late = scatter_heads(late, groups, True)
    out_part = total_of([part[:, :width] for part in late]).astype(BF16)
    late = jnp.concatenate([out_part] + [part[:, width:] for part in late], axis=1)[None]
    late = gather_items(late, 0, order_b).reshape(inner, -1)
    out_total = late[:, :width]
    by_shift = late[:, width:].reshape(inner, groups, 3, inner)
    qkv_total = jnp.stack(
        [lax.dynamic_index_in_dim(by_shift, (place - group) % groups, 1, keepdims=False) for group in range(groups)],
        axis=2,
    ).reshape(inner, 3 * width)

    back_rows = jnp.concatenate([jnp.concatenate(parts, axis=1) for parts in arrived], axis=0)
    back_norm = matmul(back_rows, jnp.concatenate(w_shifted, axis=1).T)
    _, norm_one_back = jax.vjp(layer_norm, hidden, gain_one.astype(F32))
    grad_hidden_norm, grad_gain_one = norm_one_back(back_norm)
    grad_hidden = grad_middle + grad_hidden_norm
    grad_tokens = grad_hidden.astype(BF16).reshape(item_count, span_here, width)
    grad_embed = lax.dot_general(
        onehot.astype(F32), grad_hidden, (((0,), (0,)), ((), ())), precision=lax.Precision.HIGHEST
    )
    small = jnp.concatenate([grad_embed, grad_gain_one[None], grad_gain_two[None]], axis=0)
    small = total_of(scatter_heads(small.reshape(-1, groups, inner).transpose(1, 0, 2), groups, False))
    for bit in range(bits):
        small = small + swap_items(small, bit)
    return (
        outputs,
        grad_tokens,
        small[:PASSES_MAX],
        small[PASSES_MAX],
        qkv_total.astype(F32),
        out_total.astype(F32),
        small[PASSES_MAX + 1],
        up_total.astype(F32),
        down_total.astype(F32),
    )


def solution(mesh):
    return jax.shard_map(
        layer,
        mesh=mesh,
        in_specs=(
            P("items", "heads", None),
            P("items"),
            P(),
            P(),
            P(),
            P(),
            P(),
            P(),
            P(),
            P("items", "heads", None),
        ),
        out_specs=(
            P("items", "heads", None),
            P("items", "heads", None),
            P(None, "heads"),
            P("heads"),
            P("heads", None),
            P("heads", None),
            P("heads"),
            P("heads", None),
            P("heads", None),
        ),
        check_vma=False,
    )
```

```python
import jax
import jax.numpy as jnp
from jax import lax
from jax.experimental import pallas as pl
from jax.experimental.pallas import tpu as pltpu
from jax.sharding import PartitionSpec as P


HEAD_DIM = 64
PASSES_MAX = 5
TOK_PASS = 256

epsilon = 1e-05
masked_fill = -1e30
BF16 = jnp.bfloat16
F32 = jnp.float32
NT = (((1,), (1,)), ((), ()))
VMEM_LIMIT = 56 * 1024 * 1024


def matmul(left, right):
    return jnp.dot(left, right, preferred_element_type=F32)


def layer_norm(values_in, gain):
    centered = values_in - jnp.mean(values_in, axis=-1, keepdims=True)
    spread = jnp.mean(centered * centered, axis=-1, keepdims=True)
    return centered * lax.rsqrt(spread + epsilon) * gain


def gelu_tanh(values_in):
    return jax.nn.gelu(values_in, approximate=True)


def causal(scores_t, block):
    shape = (block, block)
    allowed = lax.broadcasted_iota(jnp.int32, shape, 0) <= lax.broadcasted_iota(jnp.int32, shape, 1)
    return jnp.where(allowed, scores_t, masked_fill)


def piece_rows(place, shift, groups, span):
    return pl.ds(pl.multiple_of(lax.rem(place + shift, groups) * span, span), span)


def forward_kernel(heads_here, groups, scalars, *refs):
    own, below, above = refs[0], refs[1:groups], refs[groups:2 * groups - 1]
    embed, gain, w_here = refs[2 * groups - 1:2 * groups + 2]
    pieces = refs[2 * groups + 2:3 * groups + 2]
    normed_out, qkv, lse, tok, vt, ot, mixed = refs[3 * groups + 2:]
    block = TOK_PASS
    full_len, _ = tok.shape
    span = full_len // groups
    blocks = full_len // block
    place, count = scalars[0], scalars[1]
    inverse = 1.0 / count.astype(F32)
    embed_rows = embed.shape[0]
    inner = heads_here * HEAD_DIM

    tok[piece_rows(place, 0, groups, span), :] = own[...]
    for step in range(1, groups):

        @pl.when(place >= step)
        def _():
            tok[piece_rows(place, groups - step, groups, span), :] = below[step - 1][...]

        @pl.when(place + step < groups)
        def _():
            tok[piece_rows(place, step, groups, span), :] = above[step - 1][...]

    def project(index, carry):
        rows = pl.ds(pl.multiple_of(index * block, block), block)
        slot = lax.broadcasted_iota(jnp.int32, (block, embed_rows), 0) + index * block
        turn = jnp.floor((slot.astype(F32) + 0.5) * inverse).astype(jnp.int32)
        pass_index = slot - turn * count
        onehot = (pass_index == lax.broadcasted_iota(jnp.int32, (block, embed_rows), 1)).astype(F32)
        hidden = tok[rows, :].astype(F32) + matmul(onehot.astype(BF16), embed[...])
        normed = layer_norm(hidden, gain[...]).astype(BF16)
        normed_out[rows, :] = normed
        projected = matmul(normed, w_here[...])
        for piece in range(3 * heads_here):
            part = projected[:, piece * HEAD_DIM:(piece + 1) * HEAD_DIM]
            if piece < heads_here:
                part = part.astype(BF16).astype(F32) * HEAD_DIM ** (-0.5)
            qkv[piece, rows, :] = part.astype(BF16)
        vt[index] = projected[:, 2 * inner:].T.astype(BF16)
        return carry

    lax.fori_loop(0, blocks, project, 0)

    for at in range(blocks):
        here = slice(at * block, (at + 1) * block)

        @pl.when(at < count)
        def _():
            def one_head(head, carry):
                query = qkv[head, here, :]
                diagonal = causal(
                    lax.dot_general(qkv[heads_here + head, here, :], query, NT, preferred_element_type=F32), block
                )
                top = jnp.max(diagonal, axis=0, keepdims=True)
                if at:
                    before = lax.dot_general(
                        qkv[heads_here + head, 0:at * block, :], query, NT, preferred_element_type=F32
                    )
                    top = jnp.maximum(top, jnp.max(before, axis=0, keepdims=True))
                weight = jnp.exp(diagonal - top)
                total = jnp.sum(weight, axis=0, keepdims=True)
                head_rows = pl.ds(pl.multiple_of(head * HEAD_DIM, HEAD_DIM), HEAD_DIM)
                out = matmul(vt[at, head_rows, :], weight.astype(BF16))
                if at:
                    weight = jnp.exp(before - top)
                    total = total + jnp.sum(weight, axis=0, keepdims=True)
                    weight = weight.astype(BF16)
                    for key_at in range(at):
                        out = out + matmul(
                            vt[key_at, head_rows, :], weight[key_at * block:(key_at + 1) * block]
                        )
                ot[head_rows, :] = out * (1.0 / total)
                lse[pl.ds(head, 1), here] = top + jnp.log(total)
                return carry

            lax.fori_loop(0, heads_here, one_head, 0)
            mixed[here, :] = ot[...].T.astype(BF16)

        @pl.when(at >= count)
        def _():
            mixed[here, :] = jnp.zeros((block, inner), BF16)

    for shift in range(groups):
        pieces[shift][...] = mixed[piece_rows(place, shift, groups, span), :]


def backward_kernel(heads_here, groups, scalars, qkv, lse, *refs):
    grad_pieces, grad_qkv, outs = refs[:groups], refs[groups], refs[groups + 1:2 * groups + 1]
    grad_heads, kt, sums, grads = refs[2 * groups + 1:]
    block = TOK_PASS
    full_len = grad_qkv.shape[0]
    span = full_len // groups
    blocks = full_len // block
    place, count = scalars[0], scalars[1]

    for shift in range(groups):
        for head in range(heads_here):
            grad_heads[head, piece_rows(place, groups - shift, groups, span), :] = grad_pieces[shift][
                :, head * HEAD_DIM:(head + 1) * HEAD_DIM
            ]

    def split(index, carry):
        rows = pl.ds(pl.multiple_of(index * block, block), block)
        for head in range(heads_here):
            kt[head, index] = qkv[heads_here + head, rows, :].astype(F32).T.astype(BF16)
        return carry

    lax.fori_loop(0, blocks, split, 0)

    def one_head(head, carry):
        sums[...] = jnp.zeros_like(sums)
        for at in range(blocks):
            here = slice(at * block, (at + 1) * block)

            @pl.when(at < count)
            def _():
                query = qkv[head, here, :]
                grad = grad_heads[head, here, :]
                row_lse = lse[pl.ds(head, 1), here]
                upto = (at + 1) * block
                keys = qkv[heads_here + head, 0:upto, :]
                values = qkv[2 * heads_here + head, 0:upto, :]
                scores = lax.dot_general(keys, query, NT, preferred_element_type=F32)
                pieces = [scores[:at * block]] if at else []
                pieces.append(causal(scores[at * block:], block))
                prob = [jnp.exp(piece - row_lse) for piece in pieces]
                back = lax.dot_general(values, grad, NT, preferred_element_type=F32)
                back = ([back[:at * block]] if at else []) + [back[at * block:]]
                inner = sum(
                    jnp.sum(one * two, axis=0, keepdims=True) for one, two in zip(prob, back)
                )
                bounds = ([(0, at * block)] if at else []) + [(at * block, upto)]
                turned = None
                for (low, high), one, two in zip(bounds, prob, back):
                    shift = (one * (two - inner)).astype(BF16)
                    sums[1, low:high, :] += matmul(one.astype(BF16), grad)
                    sums[0, low:high, :] += matmul(shift, query)
                    for key_at in range(low // block, high // block):
                        part = matmul(
                            kt[head, key_at], shift[key_at * block - low:(key_at + 1) * block - low]
                        )
                        turned = part if turned is None else turned + part
                grads[head, here, :] = (turned * HEAD_DIM ** (-0.5)).T.astype(BF16)

            @pl.when(at >= count)
            def _():
                grads[head, here, :] = jnp.zeros((block, HEAD_DIM), BF16)

        grads[heads_here + head] = sums[0].astype(BF16)
        grads[2 * heads_here + head] = sums[1].astype(BF16)
        return carry

    lax.fori_loop(0, heads_here, one_head, 0)

    def join(index, carry):
        rows = pl.ds(pl.multiple_of(index * block, block), block)
        grad_qkv[rows, :] = jnp.concatenate([grads[piece, rows, :] for piece in range(3 * heads_here)], axis=1)
        return carry

    lax.fori_loop(0, blocks, join, 0)

    for shift in range(groups):
        outs[shift][...] = grad_qkv[piece_rows(place, shift, groups, span), :]


def attention_forward(scalars, own, below, above, embed_low, gain_one, w_here):
    groups = len(below) + 1
    span, width = own.shape
    full_len = span * groups
    inner = w_here.shape[1] // 3
    heads_here = inner // HEAD_DIM
    blocks = full_len // TOK_PASS
    vmem = pl.BlockSpec(memory_space=pltpu.VMEM)
    outs = pl.pallas_call(
        lambda *refs: forward_kernel(heads_here, groups, *refs),
        name="attention_forward",
        in_specs=[pl.BlockSpec(memory_space=pltpu.SMEM)] + [vmem] * (2 * groups + 2),
        out_specs=[vmem] * (groups + 3),
        scratch_shapes=[
            pltpu.VMEM((full_len, width), BF16),
            pltpu.VMEM((blocks, inner, TOK_PASS), BF16),
            pltpu.VMEM((inner, TOK_PASS), F32),
            pltpu.VMEM((full_len, inner), BF16),
        ],
        out_shape=[jax.ShapeDtypeStruct((span, inner), BF16)] * groups
        + [
            jax.ShapeDtypeStruct((full_len, width), BF16),
            jax.ShapeDtypeStruct((3 * heads_here, full_len, HEAD_DIM), BF16),
            jax.ShapeDtypeStruct((8, full_len), F32),
        ],
        compiler_params=pltpu.CompilerParams(vmem_limit_bytes=VMEM_LIMIT),
        cost_estimate=pl.CostEstimate(flops=9 * 10**9, bytes_accessed=12 * 10**6, transcendentals=3 * 10**6),
    )(scalars, own, *below, *above, embed_low, gain_one, w_here)
    return outs[:groups], outs[groups], outs[groups + 1], outs[groups + 2]


def attention_backward(scalars, qkv, lse, grad_pieces):
    groups = len(grad_pieces)
    span, inner = grad_pieces[0].shape
    full_len = span * groups
    heads_here = inner // HEAD_DIM
    blocks = full_len // TOK_PASS
    vmem = pl.BlockSpec(memory_space=pltpu.VMEM)
    outs = pl.pallas_call(
        lambda *refs: backward_kernel(heads_here, groups, *refs),
        name="attention_backward",
        in_specs=[pl.BlockSpec(memory_space=pltpu.SMEM)] + [vmem] * (groups + 2),
        out_specs=[vmem] * (groups + 1),
        scratch_shapes=[
            pltpu.VMEM((heads_here, full_len, HEAD_DIM), BF16),
            pltpu.VMEM((heads_here, blocks, HEAD_DIM, TOK_PASS), BF16),
            pltpu.VMEM((2, full_len, HEAD_DIM), F32),
            pltpu.VMEM((3 * heads_here, full_len, HEAD_DIM), BF16),
        ],
        out_shape=[jax.ShapeDtypeStruct((full_len, 3 * inner), BF16)]
        + [jax.ShapeDtypeStruct((span, 3 * inner), BF16)] * groups,
        compiler_params=pltpu.CompilerParams(vmem_limit_bytes=VMEM_LIMIT),
        cost_estimate=pl.CostEstimate(flops=9 * 10**9, bytes_accessed=8 * 10**6, transcendentals=3 * 10**6),
    )(scalars, qkv, lse, *grad_pieces)
    return outs[0], outs[1:]


def finish_kernel(groups, items, scalars, tok, embed, gain, grad_middle, *refs):
    pieces, weights = refs[:items * groups], refs[items * groups:(items + 1) * groups]
    grad_tokens, grad_embed, grad_gain = refs[(items + 1) * groups:]
    span = tok.shape[1]
    chunk = span // 2
    embed_rows = embed.shape[0]
    grad_embed[...] = jnp.zeros_like(grad_embed)
    grad_gain[...] = jnp.zeros_like(grad_gain)
    for item in range(items):
        count = scalars[1 + item]
        inverse = 1.0 / count.astype(F32)

        def rows_of(index, carry):
            rows = pl.ds(pl.multiple_of(index * chunk, chunk), chunk)
            slot = lax.broadcasted_iota(jnp.int32, (chunk, embed_rows), 0) + (scalars[0] * span + index * chunk)
            turn = jnp.floor((slot.astype(F32) + 0.5) * inverse).astype(jnp.int32)
            onehot = (slot - turn * count == lax.broadcasted_iota(jnp.int32, (chunk, embed_rows), 1)).astype(F32)
            hidden = tok[item, rows, :].astype(F32) + matmul(onehot.astype(BF16), embed[...])
            centered = hidden - jnp.mean(hidden, axis=-1, keepdims=True)
            scale = lax.rsqrt(jnp.mean(centered * centered, axis=-1, keepdims=True) + epsilon)
            normal = centered * scale
            back = lax.dot_general(pieces[item * groups][rows, :], weights[0][...], NT, preferred_element_type=F32)
            for shift in range(1, groups):
                back = back + lax.dot_general(
                    pieces[item * groups + shift][rows, :], weights[shift][...], NT, preferred_element_type=F32
                )
            grad_gain[0:1, :] += jnp.sum(back * normal, axis=0, keepdims=True)
            back = back * gain[...]
            shift_by = jnp.mean(back, axis=-1, keepdims=True)
            along = jnp.mean(back * normal, axis=-1, keepdims=True)
            grad_hidden = grad_middle[item, rows, :] + scale * (back - shift_by - normal * along)
            grad_tokens[item, rows, :] = grad_hidden.astype(BF16)
            for turn_at in range(PASSES_MAX):
                grad_embed[turn_at:turn_at + 1, :] += jnp.sum(
                    grad_hidden * onehot[:, turn_at:turn_at + 1], axis=0, keepdims=True
                )
            return carry

        lax.fori_loop(0, span // chunk, rows_of, 0)


def finish_rows(scalars, tokens, embed_low, gain_row, grad_middle, arrived, weights):
    items, span, width = tokens.shape
    groups = len(weights)
    vmem = pl.BlockSpec(memory_space=pltpu.VMEM)
    return pl.pallas_call(
        lambda *refs: finish_kernel(groups, items, *refs),
        name="finish_rows",
        in_specs=[pl.BlockSpec(memory_space=pltpu.SMEM)] + [vmem] * (4 + (items + 1) * groups),
        out_specs=[vmem] * 3,
        out_shape=[
            jax.ShapeDtypeStruct((items, span, width), BF16),
            jax.ShapeDtypeStruct((8, width), F32),
            jax.ShapeDtypeStruct((8, width), F32),
        ],
        compiler_params=pltpu.CompilerParams(vmem_limit_bytes=VMEM_LIMIT),
        cost_estimate=pl.CostEstimate(flops=3 * 10**9, bytes_accessed=12 * 10**6, transcendentals=10**3),
    )(scalars, tokens, embed_low, gain_row, grad_middle, *sum(arrived, []), *weights)


def shift_heads(piece, shift, groups):
    return lax.ppermute(piece, "heads", [(at, (at + shift) % groups) for at in range(groups)])


def swap_items(piece, bit):
    size = lax.axis_size("items")
    return lax.ppermute(piece, "items", [(at, at ^ (1 << bit)) for at in range(size)])


def item_bit(bit):
    return (lax.axis_index("items") >> bit) & 1


def halve(grad, axis, bit):
    half = grad.shape[axis] // 2
    mine = item_bit(bit)
    sent = lax.dynamic_slice_in_dim(grad, (1 - mine) * half, half, axis)
    kept = lax.dynamic_slice_in_dim(grad, mine * half, half, axis)
    return (kept.astype(F32) + swap_items(sent, bit).astype(F32)).astype(BF16)


def sum_items(grad, axis, order):
    for bit in order:
        grad = halve(grad, axis, bit)
    return grad


def gather_items(part, axis, order):
    for bit in reversed(order):
        other = swap_items(part, bit)
        high = item_bit(bit) == 1
        part = jnp.concatenate([jnp.where(high, other, part), jnp.where(high, part, other)], axis=axis)
    return part


def scatter_heads(grad, groups, static_order):
    place = lax.axis_index("heads")

    def part_for(shift):
        if static_order:
            return grad[(groups - shift) % groups]
        return lax.dynamic_index_in_dim(grad, (place + shift) % groups, 0, keepdims=False)

    return [part_for(0)] + [shift_heads(part_for(shift), shift, groups) for shift in range(1, groups)]


def total_of(parts):
    total = parts[0].astype(F32)
    for part in parts[1:]:
        total = total + part.astype(F32)
    return total


def layer(tokens, passes, embed, gain_one, w_qkv, w_out, gain_two, w_up, w_down, cotangent):
    groups = lax.axis_size("heads")
    place = lax.axis_index("heads")
    item_count, span_here, width = tokens.shape
    row_count = item_count * span_here
    inner = width // groups
    bits = lax.axis_size("items").bit_length() - 1
    order_a = list(range(bits))
    order_b = [0] + list(range(bits - 1, 0, -1))

    belows, aboves = [], []
    for item in range(item_count):
        below, above = [], []
        low = high = tokens[item]
        if item:
            low, high, *_ = lax.optimization_barrier((low, high, belows[-1][:2], aboves[-1][:2]))
        for step in range(1, groups):
            low = lax.ppermute(low, "heads", [(at, at + 1) for at in range(step - 1, groups - 1)])
            high = lax.ppermute(high, "heads", [(at, at - 1) for at in range(1, groups - step + 1)])
            below.append(low)
            above.append(high)
        belows.append(below)
        aboves.append(above)

    slot_index = place * span_here + jnp.arange(span_here, dtype=jnp.int32)
    valid_len = TOK_PASS * passes
    row_mask = (slot_index[None, :] < valid_len[:, None]).astype(F32).reshape(row_count, 1)
    pass_index = (slot_index[None, :] % passes[:, None]).reshape(row_count, 1)
    onehot = (pass_index == jnp.arange(PASSES_MAX, dtype=jnp.int32)[None, :]).astype(BF16)
    w_grouped = w_qkv.reshape(width, 3, groups, inner)

    def columns_of(shift):
        piece = lax.dynamic_index_in_dim(w_grouped, (place - shift) % groups, 2, keepdims=False)
        return piece.reshape(width, 3 * inner)

    w_shifted = [columns_of(shift) for shift in range(groups)]
    out_shifted = [
        lax.dynamic_slice_in_dim(w_out, ((place - shift) % groups) * inner, inner, 0) for shift in range(groups)
    ]
    hidden = tokens.astype(F32).reshape(row_count, width) + matmul(onehot, embed)
    grad_result = cotangent.astype(F32).reshape(row_count, width) * row_mask
    grad_low = grad_result.astype(BF16)
    grad_active = matmul(grad_low, w_down.T).astype(BF16)
    embed_low = jnp.zeros((128, width), BF16).at[:PASSES_MAX].set(embed)
    gain_row = gain_one.astype(F32)[None]

    kept, mixed_parts = [], []
    for item in range(item_count):
        scalars = jnp.stack([place, passes[item]]).astype(jnp.int32)
        pieces, normed_all, qkv, lse = attention_forward(
            scalars, tokens[item], belows[item], aboves[item], embed_low, gain_row, w_shifted[0]
        )
        kept.append((scalars, normed_all, qkv, lse))
        mixed_parts.append(
            jnp.concatenate([pieces[0]] + [shift_heads(pieces[s], s, groups) for s in range(1, groups)], axis=1)
        )

    mixed_rows = jnp.concatenate(mixed_parts, axis=0)
    middle = hidden + matmul(mixed_rows, jnp.concatenate(out_shifted, axis=0))
    second, norm_two_back = jax.vjp(layer_norm, middle, gain_two.astype(F32))
    second_low = second.astype(BF16)
    up_proj = matmul(second_low, w_up)
    active, gelu_back = jax.vjp(gelu_tanh, up_proj)
    active_low = active.astype(BF16)
    (grad_up,) = gelu_back(grad_active.astype(F32))
    grad_up_low = grad_up.astype(BF16)
    grad_middle_norm, grad_gain_two = norm_two_back(matmul(grad_up_low, w_up.T))
    grad_middle = grad_result + grad_middle_norm
    grad_branch = grad_middle.astype(BF16)
    grad_pieces = [
        matmul(grad_branch, out_shifted[(groups - shift) % groups].T).astype(BF16) for shift in range(groups)
    ]
    grad_pieces, active_low, second_low = lax.optimization_barrier((grad_pieces, active_low, second_low))
    for shift in range(1, groups):
        grad_pieces[shift] = shift_heads(grad_pieces[shift], shift, groups)

    grad_w_down = matmul(active_low.T, grad_low).astype(BF16)
    grad_w_up = matmul(second_low.T, grad_up_low).astype(BF16)
    share_down = halve(grad_w_down.reshape(groups, -1, width), 1, order_a[0])
    share_up = halve(grad_w_up.reshape(groups, inner, -1), 2, order_b[0])
    grad_pieces, share_down, share_up = lax.optimization_barrier((grad_pieces, share_down, share_up))
    share_down = halve(share_down, 1, order_a[1])
    share_up = halve(share_up, 2, order_b[1])

    flat_here, arrived = [], []
    for item in range(item_count):
        scalars, _, qkv, lse = kept[item]
        whole, pieces = attention_backward(
            scalars, qkv, lse, [piece[item * span_here:(item + 1) * span_here] for piece in grad_pieces]
        )
        flat_here.append(whole)
        parts = [pieces[0]]
        for shift in range(1, groups):
            parts.append(shift_heads(pieces[shift], shift, groups))
        arrived.append(parts)

    flat_here, share_down, share_up = lax.optimization_barrier((flat_here, share_down, share_up))
    share_down = sum_items(share_down, 1, order_a[2:])
    share_up = sum_items(share_up, 2, order_b[2:])
    grad_w_here = total_of(
        [matmul(entry[1].T, whole) for entry, whole in zip(kept, flat_here)]
    ).astype(BF16)
    grad_w_here, share_down, share_up, mixed_rows, active_low = lax.optimization_barrier(
        (grad_w_here, share_down, share_up, mixed_rows, active_low)
    )
    grad_w_out = matmul(mixed_rows.T, grad_branch).astype(BF16)
    share_down = total_of(scatter_heads(share_down, groups, False)).astype(BF16)
    share_up = total_of(scatter_heads(share_up, groups, False)).astype(BF16)

    qkv_rows = jnp.concatenate([lax.dynamic_slice_in_dim(
        grad_w_here, ((place - shift) % groups) * inner, inner, 0) for shift in range(groups)], axis=0)
    late = jnp.concatenate([grad_w_out, qkv_rows], axis=1).reshape(groups, 1 << bits, -1, width + 3 * inner)
    late = halve(late, 1, order_b[0])
    late = sum_items(late, 1, order_b[1:])[:, 0]
    late = scatter_heads(late, groups, True)
    out_part = total_of([part[:, :width] for part in late]).astype(BF16)
    late = jnp.concatenate([out_part] + [part[:, width:] for part in late], axis=1)[None]
    late = gather_items(late, 0, order_b).reshape(inner, -1)
    result = middle + matmul(active_low, w_down)
    outputs = (result * row_mask).astype(BF16).reshape(item_count, span_here, width)
    arrived, share_down, share_up, late, outputs = lax.optimization_barrier(
        (arrived, share_down, share_up, late, outputs)
    )
    down_total = gather_items(share_down, 0, order_a)
    up_total = gather_items(share_up, 1, order_b)
    out_total = late[:, :width]
    by_shift = late[:, width:].reshape(inner, groups, 3, inner)
    qkv_total = jnp.stack(
        [lax.dynamic_index_in_dim(by_shift, (place - group) % groups, 1, keepdims=False) for group in range(groups)],
        axis=2,
    ).reshape(inner, 3 * width)

    grad_tokens, grad_embed, grad_gain_one = finish_rows(
        jnp.concatenate([place[None], passes]).astype(jnp.int32),
        tokens, embed_low, gain_row, grad_middle.reshape(item_count, span_here, width), arrived, w_shifted,
    )
    small = jnp.concatenate([grad_embed[:PASSES_MAX], grad_gain_one[:1], grad_gain_two[None]], axis=0)
    small = total_of(scatter_heads(small.reshape(-1, groups, inner).transpose(1, 0, 2), groups, False))
    for bit in range(bits):
        small = small + swap_items(small, bit)
    return (
        outputs,
        grad_tokens,
        small[:PASSES_MAX],
        small[PASSES_MAX],
        qkv_total.astype(F32),
        out_total.astype(F32),
        small[PASSES_MAX + 1],
        up_total.astype(F32),
        down_total.astype(F32),
    )


def solution(mesh):
    return jax.shard_map(
        layer,
        mesh=mesh,
        in_specs=(
            P("items", "heads", None),
            P("items"),
            P(),
            P(),
            P(),
            P(),
            P(),
            P(),
            P(),
            P("items", "heads", None),
        ),
        out_specs=(
            P("items", "heads", None),
            P("items", "heads", None),
            P(None, "heads"),
            P("heads"),
            P("heads", None),
            P("heads", None),
            P("heads"),
            P("heads", None),
            P("heads", None),
        ),
        check_vma=False,
    )
```

```python
import jax
import jax.numpy as jnp
from jax import lax
from jax.experimental import pallas as pl
from jax.experimental.pallas import tpu as pltpu
from jax.sharding import PartitionSpec as P


HEAD_DIM = 64
PASSES_MAX = 5
TOK_PASS = 256

epsilon = 1e-05
masked_fill = -1e30
BF16 = jnp.bfloat16
F32 = jnp.float32
NT = (((1,), (1,)), ((), ()))
VMEM_LIMIT = 56 * 1024 * 1024


def matmul(left, right):
    return jnp.dot(left, right, preferred_element_type=F32)


def layer_norm(values_in, gain):
    centered = values_in - jnp.mean(values_in, axis=-1, keepdims=True)
    spread = jnp.mean(centered * centered, axis=-1, keepdims=True)
    return centered * lax.rsqrt(spread + epsilon) * gain


def gelu_tanh(values_in):
    return jax.nn.gelu(values_in, approximate=True)


def causal(scores_t, block):
    shape = (block, block)
    allowed = lax.broadcasted_iota(jnp.int32, shape, 0) <= lax.broadcasted_iota(jnp.int32, shape, 1)
    return jnp.where(allowed, scores_t, masked_fill)


def piece_rows(place, shift, groups, span):
    return pl.ds(pl.multiple_of(lax.rem(place + shift, groups) * span, span), span)


def forward_kernel(heads_here, groups, scalars, *refs):
    own, below, above = refs[0], refs[1:groups], refs[groups:2 * groups - 1]
    embed, gain, w_here = refs[2 * groups - 1:2 * groups + 2]
    pieces = refs[2 * groups + 2:3 * groups + 2]
    normed_out, qkv, lse, tok, vt, ot, mixed = refs[3 * groups + 2:]
    block = TOK_PASS
    full_len, _ = tok.shape
    span = full_len // groups
    blocks = full_len // block
    place, count = scalars[0], scalars[1]
    inverse = 1.0 / count.astype(F32)
    embed_rows = embed.shape[0]
    inner = heads_here * HEAD_DIM

    tok[piece_rows(place, 0, groups, span), :] = own[...]
    for step in range(1, groups):

        @pl.when(place >= step)
        def _():
            tok[piece_rows(place, groups - step, groups, span), :] = below[step - 1][...]

        @pl.when(place + step < groups)
        def _():
            tok[piece_rows(place, step, groups, span), :] = above[step - 1][...]

    def project(index, carry):
        rows = pl.ds(pl.multiple_of(index * block, block), block)
        slot = lax.broadcasted_iota(jnp.int32, (block, embed_rows), 0) + index * block
        turn = jnp.floor((slot.astype(F32) + 0.5) * inverse).astype(jnp.int32)
        pass_index = slot - turn * count
        onehot = (pass_index == lax.broadcasted_iota(jnp.int32, (block, embed_rows), 1)).astype(F32)
        hidden = tok[rows, :].astype(F32) + matmul(onehot.astype(BF16), embed[...])
        normed = layer_norm(hidden, gain[...]).astype(BF16)
        normed_out[rows, :] = normed
        projected = matmul(normed, w_here[...])
        for piece in range(3 * heads_here):
            part = projected[:, piece * HEAD_DIM:(piece + 1) * HEAD_DIM]
            if piece < heads_here:
                part = part.astype(BF16).astype(F32) * HEAD_DIM ** (-0.5)
            qkv[piece, rows, :] = part.astype(BF16)
        vt[index] = projected[:, 2 * inner:].T.astype(BF16)
        return carry

    lax.fori_loop(0, blocks, project, 0)

    for at in range(blocks):
        here = slice(at * block, (at + 1) * block)

        @pl.when(at < count)
        def _():
            def one_head(head, carry):
                query = qkv[head, here, :]
                diagonal = causal(
                    lax.dot_general(qkv[heads_here + head, here, :], query, NT, preferred_element_type=F32), block
                )
                top = jnp.max(diagonal, axis=0, keepdims=True)
                if at:
                    before = lax.dot_general(
                        qkv[heads_here + head, 0:at * block, :], query, NT, preferred_element_type=F32
                    )
                    top = jnp.maximum(top, jnp.max(before, axis=0, keepdims=True))
                weight = jnp.exp(diagonal - top)
                total = jnp.sum(weight, axis=0, keepdims=True)
                head_rows = pl.ds(pl.multiple_of(head * HEAD_DIM, HEAD_DIM), HEAD_DIM)
                out = matmul(vt[at, head_rows, :], weight.astype(BF16))
                if at:
                    weight = jnp.exp(before - top)
                    total = total + jnp.sum(weight, axis=0, keepdims=True)
                    weight = weight.astype(BF16)
                    for key_at in range(at):
                        out = out + matmul(
                            vt[key_at, head_rows, :], weight[key_at * block:(key_at + 1) * block]
                        )
                ot[head_rows, :] = out * (1.0 / total)
                lse[pl.ds(head, 1), here] = top + jnp.log(total)
                return carry

            lax.fori_loop(0, heads_here, one_head, 0)
            mixed[here, :] = ot[...].T.astype(BF16)

        @pl.when(at >= count)
        def _():
            mixed[here, :] = jnp.zeros((block, inner), BF16)

    for shift in range(groups):
        pieces[shift][...] = mixed[piece_rows(place, shift, groups, span), :]


def backward_kernel(heads_here, groups, scalars, qkv, lse, *refs):
    grad_pieces, grad_qkv, outs = refs[:groups], refs[groups], refs[groups + 1:2 * groups + 1]
    grad_heads, kt, sums, grads = refs[2 * groups + 1:]
    block = TOK_PASS
    full_len = grad_qkv.shape[0]
    span = full_len // groups
    blocks = full_len // block
    place, count = scalars[0], scalars[1]

    for shift in range(groups):
        for head in range(heads_here):
            grad_heads[head, piece_rows(place, groups - shift, groups, span), :] = grad_pieces[shift][
                :, head * HEAD_DIM:(head + 1) * HEAD_DIM
            ]

    def split(index, carry):
        rows = pl.ds(pl.multiple_of(index * block, block), block)
        for head in range(heads_here):
            kt[head, index] = qkv[heads_here + head, rows, :].astype(F32).T.astype(BF16)
        return carry

    lax.fori_loop(0, blocks, split, 0)

    def one_head(head, carry):
        sums[...] = jnp.zeros_like(sums)
        for at in range(blocks):
            here = slice(at * block, (at + 1) * block)

            @pl.when(at < count)
            def _():
                query = qkv[head, here, :]
                grad = grad_heads[head, here, :]
                row_lse = lse[pl.ds(head, 1), here]
                upto = (at + 1) * block
                keys = qkv[heads_here + head, 0:upto, :]
                values = qkv[2 * heads_here + head, 0:upto, :]
                scores = lax.dot_general(keys, query, NT, preferred_element_type=F32)
                pieces = [scores[:at * block]] if at else []
                pieces.append(causal(scores[at * block:], block))
                prob = [jnp.exp(piece - row_lse) for piece in pieces]
                back = lax.dot_general(values, grad, NT, preferred_element_type=F32)
                back = ([back[:at * block]] if at else []) + [back[at * block:]]
                inner = sum(
                    jnp.sum(one * two, axis=0, keepdims=True) for one, two in zip(prob, back)
                )
                bounds = ([(0, at * block)] if at else []) + [(at * block, upto)]
                turned = None
                for (low, high), one, two in zip(bounds, prob, back):
                    shift = (one * (two - inner)).astype(BF16)
                    sums[1, low:high, :] += matmul(one.astype(BF16), grad)
                    sums[0, low:high, :] += matmul(shift, query)
                    for key_at in range(low // block, high // block):
                        part = matmul(
                            kt[head, key_at], shift[key_at * block - low:(key_at + 1) * block - low]
                        )
                        turned = part if turned is None else turned + part
                grads[head, here, :] = (turned * HEAD_DIM ** (-0.5)).T.astype(BF16)

            @pl.when(at >= count)
            def _():
                grads[head, here, :] = jnp.zeros((block, HEAD_DIM), BF16)

        grads[heads_here + head] = sums[0].astype(BF16)
        grads[2 * heads_here + head] = sums[1].astype(BF16)
        return carry

    lax.fori_loop(0, heads_here, one_head, 0)

    def join(index, carry):
        rows = pl.ds(pl.multiple_of(index * block, block), block)
        grad_qkv[rows, :] = jnp.concatenate([grads[piece, rows, :] for piece in range(3 * heads_here)], axis=1)
        return carry

    lax.fori_loop(0, blocks, join, 0)

    for shift in range(groups):
        outs[shift][...] = grad_qkv[piece_rows(place, shift, groups, span), :]


def attention_forward(scalars, own, below, above, embed_low, gain_one, w_here):
    groups = len(below) + 1
    span, width = own.shape
    full_len = span * groups
    inner = w_here.shape[1] // 3
    heads_here = inner // HEAD_DIM
    blocks = full_len // TOK_PASS
    vmem = pl.BlockSpec(memory_space=pltpu.VMEM)
    outs = pl.pallas_call(
        lambda *refs: forward_kernel(heads_here, groups, *refs),
        name="attention_forward",
        in_specs=[pl.BlockSpec(memory_space=pltpu.SMEM)] + [vmem] * (2 * groups + 2),
        out_specs=[vmem] * (groups + 3),
        scratch_shapes=[
            pltpu.VMEM((full_len, width), BF16),
            pltpu.VMEM((blocks, inner, TOK_PASS), BF16),
            pltpu.VMEM((inner, TOK_PASS), F32),
            pltpu.VMEM((full_len, inner), BF16),
        ],
        out_shape=[jax.ShapeDtypeStruct((span, inner), BF16)] * groups
        + [
            jax.ShapeDtypeStruct((full_len, width), BF16),
            jax.ShapeDtypeStruct((3 * heads_here, full_len, HEAD_DIM), BF16),
            jax.ShapeDtypeStruct((8, full_len), F32),
        ],
        compiler_params=pltpu.CompilerParams(vmem_limit_bytes=VMEM_LIMIT),
        cost_estimate=pl.CostEstimate(flops=9 * 10**9, bytes_accessed=12 * 10**6, transcendentals=3 * 10**6),
    )(scalars, own, *below, *above, embed_low, gain_one, w_here)
    return outs[:groups], outs[groups], outs[groups + 1], outs[groups + 2]


def attention_backward(scalars, qkv, lse, grad_pieces):
    groups = len(grad_pieces)
    span, inner = grad_pieces[0].shape
    full_len = span * groups
    heads_here = inner // HEAD_DIM
    blocks = full_len // TOK_PASS
    vmem = pl.BlockSpec(memory_space=pltpu.VMEM)
    outs = pl.pallas_call(
        lambda *refs: backward_kernel(heads_here, groups, *refs),
        name="attention_backward",
        in_specs=[pl.BlockSpec(memory_space=pltpu.SMEM)] + [vmem] * (groups + 2),
        out_specs=[vmem] * (groups + 1),
        scratch_shapes=[
            pltpu.VMEM((heads_here, full_len, HEAD_DIM), BF16),
            pltpu.VMEM((heads_here, blocks, HEAD_DIM, TOK_PASS), BF16),
            pltpu.VMEM((2, full_len, HEAD_DIM), F32),
            pltpu.VMEM((3 * heads_here, full_len, HEAD_DIM), BF16),
        ],
        out_shape=[jax.ShapeDtypeStruct((full_len, 3 * inner), BF16)]
        + [jax.ShapeDtypeStruct((span, 3 * inner), BF16)] * groups,
        compiler_params=pltpu.CompilerParams(vmem_limit_bytes=VMEM_LIMIT),
        cost_estimate=pl.CostEstimate(flops=9 * 10**9, bytes_accessed=8 * 10**6, transcendentals=3 * 10**6),
    )(scalars, qkv, lse, *grad_pieces)
    return outs[0], outs[1:]


def finish_kernel(groups, items, scalars, tok, embed, gain, grad_middle, *refs):
    pieces, weights = refs[:items * groups], refs[items * groups:(items + 1) * groups]
    grad_tokens, grad_embed, grad_gain = refs[(items + 1) * groups:]
    span = tok.shape[1]
    chunk = span // 2
    embed_rows = embed.shape[0]
    grad_embed[...] = jnp.zeros_like(grad_embed)
    grad_gain[...] = jnp.zeros_like(grad_gain)
    for item in range(items):
        count = scalars[1 + item]
        inverse = 1.0 / count.astype(F32)

        def rows_of(index, carry):
            rows = pl.ds(pl.multiple_of(index * chunk, chunk), chunk)
            slot = lax.broadcasted_iota(jnp.int32, (chunk, embed_rows), 0) + (scalars[0] * span + index * chunk)
            turn = jnp.floor((slot.astype(F32) + 0.5) * inverse).astype(jnp.int32)
            onehot = (slot - turn * count == lax.broadcasted_iota(jnp.int32, (chunk, embed_rows), 1)).astype(F32)
            hidden = tok[item, rows, :].astype(F32) + matmul(onehot.astype(BF16), embed[...])
            centered = hidden - jnp.mean(hidden, axis=-1, keepdims=True)
            scale = lax.rsqrt(jnp.mean(centered * centered, axis=-1, keepdims=True) + epsilon)
            normal = centered * scale
            back = lax.dot_general(pieces[item * groups][rows, :], weights[0][...], NT, preferred_element_type=F32)
            for shift in range(1, groups):
                back = back + lax.dot_general(
                    pieces[item * groups + shift][rows, :], weights[shift][...], NT, preferred_element_type=F32
                )
            grad_gain[0:1, :] += jnp.sum(back * normal, axis=0, keepdims=True)
            back = back * gain[...]
            shift_by = jnp.mean(back, axis=-1, keepdims=True)
            along = jnp.mean(back * normal, axis=-1, keepdims=True)
            grad_hidden = grad_middle[item, rows, :] + scale * (back - shift_by - normal * along)
            grad_tokens[item, rows, :] = grad_hidden.astype(BF16)
            for turn_at in range(PASSES_MAX):
                grad_embed[turn_at:turn_at + 1, :] += jnp.sum(
                    grad_hidden * onehot[:, turn_at:turn_at + 1], axis=0, keepdims=True
                )
            return carry

        lax.fori_loop(0, span // chunk, rows_of, 0)


def finish_rows(scalars, tokens, embed_low, gain_row, grad_middle, arrived, weights):
    items, span, width = tokens.shape
    groups = len(weights)
    vmem = pl.BlockSpec(memory_space=pltpu.VMEM)
    return pl.pallas_call(
        lambda *refs: finish_kernel(groups, items, *refs),
        name="finish_rows",
        in_specs=[pl.BlockSpec(memory_space=pltpu.SMEM)] + [vmem] * (4 + (items + 1) * groups),
        out_specs=[vmem] * 3,
        out_shape=[
            jax.ShapeDtypeStruct((items, span, width), BF16),
            jax.ShapeDtypeStruct((8, width), F32),
            jax.ShapeDtypeStruct((8, width), F32),
        ],
        compiler_params=pltpu.CompilerParams(vmem_limit_bytes=VMEM_LIMIT),
        cost_estimate=pl.CostEstimate(flops=3 * 10**9, bytes_accessed=12 * 10**6, transcendentals=10**3),
    )(scalars, tokens, embed_low, gain_row, grad_middle, *sum(arrived, []), *weights)


def shift_heads(piece, shift, groups):
    return lax.ppermute(piece, "heads", [(at, (at + shift) % groups) for at in range(groups)])


def swap_items(piece, bit):
    size = lax.axis_size("items")
    return lax.ppermute(piece, "items", [(at, at ^ (1 << bit)) for at in range(size)])


def item_bit(bit):
    return (lax.axis_index("items") >> bit) & 1


def halve(grad, axis, bit):
    half = grad.shape[axis] // 2
    mine = item_bit(bit)
    sent = lax.dynamic_slice_in_dim(grad, (1 - mine) * half, half, axis)
    kept = lax.dynamic_slice_in_dim(grad, mine * half, half, axis)
    return (kept.astype(F32) + swap_items(sent, bit).astype(F32)).astype(BF16)


def sum_items(grad, axis, order):
    for bit in order:
        grad = halve(grad, axis, bit)
    return grad


def gather_items(part, axis, order):
    for bit in reversed(order):
        other = swap_items(part, bit)
        high = item_bit(bit) == 1
        part = jnp.concatenate([jnp.where(high, other, part), jnp.where(high, part, other)], axis=axis)
    return part


def scatter_heads(grad, groups, static_order):
    place = lax.axis_index("heads")

    def part_for(shift):
        if static_order:
            return grad[(groups - shift) % groups]
        return lax.dynamic_index_in_dim(grad, (place + shift) % groups, 0, keepdims=False)

    parts = [part_for(0)]
    for shift in range(1, groups):
        parts.append(shift_heads(part_for(shift), shift, groups))
    return parts


def total_of(parts):
    total = parts[0].astype(F32)
    for part in parts[1:]:
        total = total + part.astype(F32)
    return total


def layer(tokens, passes, embed, gain_one, w_qkv, w_out, gain_two, w_up, w_down, cotangent):
    groups = lax.axis_size("heads")
    place = lax.axis_index("heads")
    item_count, span_here, width = tokens.shape
    row_count = item_count * span_here
    inner = width // groups
    bits = lax.axis_size("items").bit_length() - 1
    order_a = list(range(bits))
    order_b = [0] + list(range(bits - 1, 0, -1))

    belows, aboves = [], []
    for item in range(item_count):
        below, above = [], []
        low = high = tokens[item]
        for step in range(1, groups):
            low = lax.ppermute(low, "heads", [(at, at + 1) for at in range(step - 1, groups - 1)])
            high = lax.ppermute(high, "heads", [(at, at - 1) for at in range(1, groups - step + 1)])
            below.append(low)
            above.append(high)
        belows.append(below)
        aboves.append(above)

    slot_index = place * span_here + jnp.arange(span_here, dtype=jnp.int32)
    valid_len = TOK_PASS * passes
    row_mask = (slot_index[None, :] < valid_len[:, None]).astype(F32).reshape(row_count, 1)
    pass_index = (slot_index[None, :] % passes[:, None]).reshape(row_count, 1)
    onehot = (pass_index == jnp.arange(PASSES_MAX, dtype=jnp.int32)[None, :]).astype(BF16)
    w_grouped = w_qkv.reshape(width, 3, groups, inner)

    def columns_of(shift):
        piece = lax.dynamic_index_in_dim(w_grouped, (place - shift) % groups, 2, keepdims=False)
        return piece.reshape(width, 3 * inner)

    w_shifted = [columns_of(shift) for shift in range(groups)]
    out_shifted = [
        lax.dynamic_slice_in_dim(w_out, ((place - shift) % groups) * inner, inner, 0) for shift in range(groups)
    ]
    hidden = tokens.astype(F32).reshape(row_count, width) + matmul(onehot, embed)
    grad_result = cotangent.astype(F32).reshape(row_count, width) * row_mask
    grad_low = grad_result.astype(BF16)
    grad_active = matmul(grad_low, w_down.T).astype(BF16)
    embed_low = jnp.zeros((128, width), BF16).at[:PASSES_MAX].set(embed)
    gain_row = gain_one.astype(F32)[None]
    w_shifted, out_shifted, grad_active = lax.optimization_barrier((w_shifted, out_shifted, grad_active))

    kept, mixed_parts = [], []
    for item in range(item_count):
        scalars = jnp.stack([place, passes[item]]).astype(jnp.int32)
        pieces, normed_all, qkv, lse = attention_forward(
            scalars, tokens[item], belows[item], aboves[item], embed_low, gain_row, w_shifted[0]
        )
        kept.append((scalars, normed_all, qkv, lse))
        mixed_parts.append(
            jnp.concatenate([pieces[0]] + [shift_heads(pieces[s], s, groups) for s in range(1, groups)], axis=1)
        )

    mixed_rows = jnp.concatenate(mixed_parts, axis=0)
    middle = hidden + matmul(mixed_rows, jnp.concatenate(out_shifted, axis=0))
    second, norm_two_back = jax.vjp(layer_norm, middle, gain_two.astype(F32))
    second_low = second.astype(BF16)
    up_proj = matmul(second_low, w_up)
    active, gelu_back = jax.vjp(gelu_tanh, up_proj)
    active_low = active.astype(BF16)
    (grad_up,) = gelu_back(grad_active.astype(F32))
    grad_up_low = grad_up.astype(BF16)
    grad_middle_norm, grad_gain_two = norm_two_back(matmul(grad_up_low, w_up.T))
    grad_middle = grad_result + grad_middle_norm
    grad_branch = grad_middle.astype(BF16)
    grad_pieces = [
        matmul(grad_branch, out_shifted[(groups - shift) % groups].T).astype(BF16) for shift in range(groups)
    ]
    grad_pieces, active_low, second_low = lax.optimization_barrier((grad_pieces, active_low, second_low))
    for shift in range(1, groups):
        grad_pieces[shift] = shift_heads(grad_pieces[shift], shift, groups)

    grad_w_down = matmul(active_low.T, grad_low).astype(BF16)
    grad_w_up = matmul(second_low.T, grad_up_low).astype(BF16)
    share_down = halve(grad_w_down.reshape(groups, -1, width), 1, order_a[0])
    share_up = halve(grad_w_up.reshape(groups, inner, -1), 2, order_b[0])
    grad_pieces, share_down, share_up = lax.optimization_barrier((grad_pieces, share_down, share_up))
    share_down = halve(share_down, 1, order_a[1])
    share_up = halve(share_up, 2, order_b[1])

    flat_here, arrived = [], []
    for item in range(item_count):
        scalars, _, qkv, lse = kept[item]
        whole, pieces = attention_backward(
            scalars, qkv, lse, [piece[item * span_here:(item + 1) * span_here] for piece in grad_pieces]
        )
        flat_here.append(whole)
        parts = [pieces[0]]
        for shift in range(1, groups):
            parts.append(shift_heads(pieces[shift], shift, groups))
        arrived.append(parts)

    flat_here, share_down, share_up = lax.optimization_barrier((flat_here, share_down, share_up))
    share_down = sum_items(share_down, 1, order_a[2:])
    share_up = sum_items(share_up, 2, order_b[2:])
    grad_w_here = total_of(
        [matmul(entry[1].T, whole) for entry, whole in zip(kept, flat_here)]
    ).astype(BF16)
    grad_w_here, share_down, share_up, mixed_rows, active_low = lax.optimization_barrier(
        (grad_w_here, share_down, share_up, mixed_rows, active_low)
    )
    grad_w_out = matmul(mixed_rows.T, grad_branch).astype(BF16)
    share_down = total_of(scatter_heads(share_down, groups, False)).astype(BF16)
    share_up = total_of(scatter_heads(share_up, groups, False)).astype(BF16)

    qkv_rows = jnp.concatenate(
        [
            lax.dynamic_slice_in_dim(grad_w_here, ((place - shift) % groups) * inner, inner, 0)
            for shift in range(groups)
        ],
        axis=0,
    )
    late = jnp.concatenate([grad_w_out, qkv_rows], axis=1)
    late = late.reshape(groups, 1 << bits, -1, width + 3 * inner)
    late = sum_items(late, 1, order_b)[:, 0]
    result = middle + matmul(active_low, w_down)
    outputs = (result * row_mask).astype(BF16).reshape(item_count, span_here, width)
    late = scatter_heads(late, groups, True)
    arrived, share_down, share_up, outputs = lax.optimization_barrier(
        (arrived, share_down, share_up, outputs)
    )
    down_total = gather_items(share_down, 0, order_a)
    up_total = gather_items(share_up, 1, order_b)
    out_part = total_of([part[:, :width] for part in late]).astype(BF16)
    late = jnp.concatenate([out_part] + [part[:, width:] for part in late], axis=1)[None]
    late = gather_items(late, 0, order_b).reshape(inner, -1)
    out_total = late[:, :width]
    by_shift = late[:, width:].reshape(inner, groups, 3, inner)
    qkv_total = jnp.stack(
        [lax.dynamic_index_in_dim(by_shift, (place - group) % groups, 1, keepdims=False) for group in range(groups)],
        axis=2,
    ).reshape(inner, 3 * width)

    grad_tokens, grad_embed, grad_gain_one = finish_rows(
        jnp.concatenate([place[None], passes]).astype(jnp.int32),
        tokens, embed_low, gain_row, grad_middle.reshape(item_count, span_here, width), arrived, w_shifted,
    )
    small = jnp.concatenate([grad_embed[:PASSES_MAX], grad_gain_one[:1], grad_gain_two[None]], axis=0)
    small = total_of(scatter_heads(small.reshape(-1, groups, inner).transpose(1, 0, 2), groups, False))
    for bit in range(bits):
        small = small + swap_items(small, bit)
    return (
        outputs,
        grad_tokens,
        small[:PASSES_MAX],
        small[PASSES_MAX],
        qkv_total.astype(F32),
        out_total.astype(F32),
        small[PASSES_MAX + 1],
        up_total.astype(F32),
        down_total.astype(F32),
    )


def solution(mesh):
    return jax.shard_map(
        layer,
        mesh=mesh,
        in_specs=(
            P("items", "heads", None),
            P("items"),
            P(),
            P(),
            P(),
            P(),
            P(),
            P(),
            P(),
            P("items", "heads", None),
        ),
        out_specs=(
            P("items", "heads", None),
            P("items", "heads", None),
            P(None, "heads"),
            P("heads"),
            P("heads", None),
            P("heads", None),
            P("heads"),
            P("heads", None),
            P("heads", None),
        ),
        check_vma=False,
    )
```

```python
import jax
import jax.numpy as jnp
from jax import lax
from jax.experimental import pallas as pl
from jax.experimental.pallas import tpu as pltpu
from jax.sharding import PartitionSpec as P


HEAD_DIM = 64
PASSES_MAX = 5
TOK_PASS = 256

epsilon = 1e-05
masked_fill = -1e30
BF16 = jnp.bfloat16
F32 = jnp.float32
NT = (((1,), (1,)), ((), ()))
VMEM_LIMIT = 56 * 1024 * 1024


def matmul(left, right):
    return jnp.dot(left, right, preferred_element_type=F32)


def layer_norm(values_in, gain):
    centered = values_in - jnp.mean(values_in, axis=-1, keepdims=True)
    spread = jnp.mean(centered * centered, axis=-1, keepdims=True)
    return centered * lax.rsqrt(spread + epsilon) * gain


def gelu_tanh(values_in):
    return jax.nn.gelu(values_in, approximate=True)


def causal(scores_t, block):
    shape = (block, block)
    allowed = lax.broadcasted_iota(jnp.int32, shape, 0) <= lax.broadcasted_iota(jnp.int32, shape, 1)
    return jnp.where(allowed, scores_t, masked_fill)


def piece_rows(place, shift, groups, span):
    return pl.ds(pl.multiple_of(lax.rem(place + shift, groups) * span, span), span)


def forward_kernel(heads_here, groups, scalars, *refs):
    own, below, above = refs[0], refs[1:groups], refs[groups:2 * groups - 1]
    embed, gain, w_here = refs[2 * groups - 1:2 * groups + 2]
    pieces = refs[2 * groups + 2:3 * groups + 2]
    normed_out, qkv, lse, tok, vt, ot, mixed = refs[3 * groups + 2:]
    block = TOK_PASS
    full_len, _ = tok.shape
    span = full_len // groups
    blocks = full_len // block
    place, count = scalars[0], scalars[1]
    inverse = 1.0 / count.astype(F32)
    embed_rows = embed.shape[0]
    inner = heads_here * HEAD_DIM

    tok[piece_rows(place, 0, groups, span), :] = own[...]
    for step in range(1, groups):

        @pl.when(place >= step)
        def _():
            tok[piece_rows(place, groups - step, groups, span), :] = below[step - 1][...]

        @pl.when(place + step < groups)
        def _():
            tok[piece_rows(place, step, groups, span), :] = above[step - 1][...]

    def project(index, carry):
        rows = pl.ds(pl.multiple_of(index * block, block), block)
        slot = lax.broadcasted_iota(jnp.int32, (block, embed_rows), 0) + index * block
        turn = jnp.floor((slot.astype(F32) + 0.5) * inverse).astype(jnp.int32)
        pass_index = slot - turn * count
        onehot = (pass_index == lax.broadcasted_iota(jnp.int32, (block, embed_rows), 1)).astype(F32)
        hidden = tok[rows, :].astype(F32) + matmul(onehot.astype(BF16), embed[...])
        normed = layer_norm(hidden, gain[...]).astype(BF16)
        normed_out[rows, :] = normed
        projected = matmul(normed, w_here[...])
        for piece in range(3 * heads_here):
            part = projected[:, piece * HEAD_DIM:(piece + 1) * HEAD_DIM]
            if piece < heads_here:
                part = part.astype(BF16).astype(F32) * HEAD_DIM ** (-0.5)
            qkv[piece, rows, :] = part.astype(BF16)
        vt[index] = projected[:, 2 * inner:].T.astype(BF16)
        return carry

    lax.fori_loop(0, blocks, project, 0)

    for at in range(blocks):
        here = slice(at * block, (at + 1) * block)

        @pl.when(at < count)
        def _():
            def one_head(head, carry):
                query = qkv[head, here, :]
                diagonal = causal(
                    lax.dot_general(qkv[heads_here + head, here, :], query, NT, preferred_element_type=F32), block
                )
                top = jnp.max(diagonal, axis=0, keepdims=True)
                if at:
                    before = lax.dot_general(
                        qkv[heads_here + head, 0:at * block, :], query, NT, preferred_element_type=F32
                    )
                    top = jnp.maximum(top, jnp.max(before, axis=0, keepdims=True))
                weight = jnp.exp(diagonal - top)
                total = jnp.sum(weight, axis=0, keepdims=True)
                head_rows = pl.ds(pl.multiple_of(head * HEAD_DIM, HEAD_DIM), HEAD_DIM)
                out = matmul(vt[at, head_rows, :], weight.astype(BF16))
                if at:
                    weight = jnp.exp(before - top)
                    total = total + jnp.sum(weight, axis=0, keepdims=True)
                    weight = weight.astype(BF16)
                    for key_at in range(at):
                        out = out + matmul(
                            vt[key_at, head_rows, :], weight[key_at * block:(key_at + 1) * block]
                        )
                ot[head_rows, :] = out * (1.0 / total)
                lse[pl.ds(head, 1), here] = top + jnp.log(total)
                return carry

            lax.fori_loop(0, heads_here, one_head, 0)
            mixed[here, :] = ot[...].T.astype(BF16)

        @pl.when(at >= count)
        def _():
            mixed[here, :] = jnp.zeros((block, inner), BF16)

    for shift in range(groups):
        pieces[shift][...] = mixed[piece_rows(place, shift, groups, span), :]


def backward_kernel(heads_here, groups, scalars, qkv, lse, *refs):
    grad_pieces, grad_qkv, outs = refs[:groups], refs[groups], refs[groups + 1:2 * groups + 1]
    grad_heads, kt, sums, grads = refs[2 * groups + 1:]
    block = TOK_PASS
    full_len = grad_qkv.shape[0]
    span = full_len // groups
    blocks = full_len // block
    place, count = scalars[0], scalars[1]

    for shift in range(groups):
        for head in range(heads_here):
            grad_heads[head, piece_rows(place, groups - shift, groups, span), :] = grad_pieces[shift][
                :, head * HEAD_DIM:(head + 1) * HEAD_DIM
            ]

    def split(index, carry):
        rows = pl.ds(pl.multiple_of(index * block, block), block)
        for head in range(heads_here):
            kt[head, index] = qkv[heads_here + head, rows, :].astype(F32).T.astype(BF16)
        return carry

    lax.fori_loop(0, blocks, split, 0)

    def one_head(head, carry):
        sums[...] = jnp.zeros_like(sums)
        for at in range(blocks):
            here = slice(at * block, (at + 1) * block)

            @pl.when(at < count)
            def _():
                query = qkv[head, here, :]
                grad = grad_heads[head, here, :]
                row_lse = lse[pl.ds(head, 1), here]
                upto = (at + 1) * block
                keys = qkv[heads_here + head, 0:upto, :]
                values = qkv[2 * heads_here + head, 0:upto, :]
                scores = lax.dot_general(keys, query, NT, preferred_element_type=F32)
                pieces = [scores[:at * block]] if at else []
                pieces.append(causal(scores[at * block:], block))
                prob = [jnp.exp(piece - row_lse) for piece in pieces]
                back = lax.dot_general(values, grad, NT, preferred_element_type=F32)
                back = ([back[:at * block]] if at else []) + [back[at * block:]]
                inner = sum(
                    jnp.sum(one * two, axis=0, keepdims=True) for one, two in zip(prob, back)
                )
                bounds = ([(0, at * block)] if at else []) + [(at * block, upto)]
                turned = None
                for (low, high), one, two in zip(bounds, prob, back):
                    shift = (one * (two - inner)).astype(BF16)
                    sums[1, low:high, :] += matmul(one.astype(BF16), grad)
                    sums[0, low:high, :] += matmul(shift, query)
                    for key_at in range(low // block, high // block):
                        part = matmul(
                            kt[head, key_at], shift[key_at * block - low:(key_at + 1) * block - low]
                        )
                        turned = part if turned is None else turned + part
                grads[head, here, :] = (turned * HEAD_DIM ** (-0.5)).T.astype(BF16)

            @pl.when(at >= count)
            def _():
                grads[head, here, :] = jnp.zeros((block, HEAD_DIM), BF16)

        grads[heads_here + head] = sums[0].astype(BF16)
        grads[2 * heads_here + head] = sums[1].astype(BF16)
        return carry

    lax.fori_loop(0, heads_here, one_head, 0)

    def join(index, carry):
        rows = pl.ds(pl.multiple_of(index * block, block), block)
        grad_qkv[rows, :] = jnp.concatenate([grads[piece, rows, :] for piece in range(3 * heads_here)], axis=1)
        return carry

    lax.fori_loop(0, blocks, join, 0)

    for shift in range(groups):
        outs[shift][...] = grad_qkv[piece_rows(place, shift, groups, span), :]


def attention_forward(scalars, own, below, above, embed_low, gain_one, w_here):
    groups = len(below) + 1
    span, width = own.shape
    full_len = span * groups
    inner = w_here.shape[1] // 3
    heads_here = inner // HEAD_DIM
    blocks = full_len // TOK_PASS
    vmem = pl.BlockSpec(memory_space=pltpu.VMEM)
    outs = pl.pallas_call(
        lambda *refs: forward_kernel(heads_here, groups, *refs),
        name="attention_forward",
        in_specs=[pl.BlockSpec(memory_space=pltpu.SMEM)] + [vmem] * (2 * groups + 2),
        out_specs=[vmem] * (groups + 3),
        scratch_shapes=[
            pltpu.VMEM((full_len, width), BF16),
            pltpu.VMEM((blocks, inner, TOK_PASS), BF16),
            pltpu.VMEM((inner, TOK_PASS), F32),
            pltpu.VMEM((full_len, inner), BF16),
        ],
        out_shape=[jax.ShapeDtypeStruct((span, inner), BF16)] * groups
        + [
            jax.ShapeDtypeStruct((full_len, width), BF16),
            jax.ShapeDtypeStruct((3 * heads_here, full_len, HEAD_DIM), BF16),
            jax.ShapeDtypeStruct((8, full_len), F32),
        ],
        compiler_params=pltpu.CompilerParams(vmem_limit_bytes=VMEM_LIMIT),
        cost_estimate=pl.CostEstimate(flops=9 * 10**9, bytes_accessed=12 * 10**6, transcendentals=3 * 10**6),
    )(scalars, own, *below, *above, embed_low, gain_one, w_here)
    return outs[:groups], outs[groups], outs[groups + 1], outs[groups + 2]


def attention_backward(scalars, qkv, lse, grad_pieces):
    groups = len(grad_pieces)
    span, inner = grad_pieces[0].shape
    full_len = span * groups
    heads_here = inner // HEAD_DIM
    blocks = full_len // TOK_PASS
    vmem = pl.BlockSpec(memory_space=pltpu.VMEM)
    outs = pl.pallas_call(
        lambda *refs: backward_kernel(heads_here, groups, *refs),
        name="attention_backward",
        in_specs=[pl.BlockSpec(memory_space=pltpu.SMEM)] + [vmem] * (groups + 2),
        out_specs=[vmem] * (groups + 1),
        scratch_shapes=[
            pltpu.VMEM((heads_here, full_len, HEAD_DIM), BF16),
            pltpu.VMEM((heads_here, blocks, HEAD_DIM, TOK_PASS), BF16),
            pltpu.VMEM((2, full_len, HEAD_DIM), F32),
            pltpu.VMEM((3 * heads_here, full_len, HEAD_DIM), BF16),
        ],
        out_shape=[jax.ShapeDtypeStruct((full_len, 3 * inner), BF16)]
        + [jax.ShapeDtypeStruct((span, 3 * inner), BF16)] * groups,
        compiler_params=pltpu.CompilerParams(vmem_limit_bytes=VMEM_LIMIT),
        cost_estimate=pl.CostEstimate(flops=9 * 10**9, bytes_accessed=8 * 10**6, transcendentals=3 * 10**6),
    )(scalars, qkv, lse, *grad_pieces)
    return outs[0], outs[1:]


def finish_kernel(groups, items, scalars, tok, embed, gain, grad_middle, *refs):
    pieces, weights = refs[:items * groups], refs[items * groups:(items + 1) * groups]
    grad_tokens, grad_embed, grad_gain = refs[(items + 1) * groups:]
    span = tok.shape[1]
    chunk = span // 2
    embed_rows = embed.shape[0]
    grad_embed[...] = jnp.zeros_like(grad_embed)
    grad_gain[...] = jnp.zeros_like(grad_gain)
    for item in range(items):
        count = scalars[1 + item]
        inverse = 1.0 / count.astype(F32)

        def rows_of(index, carry):
            rows = pl.ds(pl.multiple_of(index * chunk, chunk), chunk)
            slot = lax.broadcasted_iota(jnp.int32, (chunk, embed_rows), 0) + (scalars[0] * span + index * chunk)
            turn = jnp.floor((slot.astype(F32) + 0.5) * inverse).astype(jnp.int32)
            onehot = (slot - turn * count == lax.broadcasted_iota(jnp.int32, (chunk, embed_rows), 1)).astype(F32)
            hidden = tok[item, rows, :].astype(F32) + matmul(onehot.astype(BF16), embed[...])
            centered = hidden - jnp.mean(hidden, axis=-1, keepdims=True)
            scale = lax.rsqrt(jnp.mean(centered * centered, axis=-1, keepdims=True) + epsilon)
            normal = centered * scale
            back = matmul(pieces[item * groups][rows, :], weights[0][...])
            for shift in range(1, groups):
                back = back + matmul(pieces[item * groups + shift][rows, :], weights[shift][...])
            grad_gain[0:1, :] += jnp.sum(back * normal, axis=0, keepdims=True)
            back = back * gain[...]
            shift_by = jnp.mean(back, axis=-1, keepdims=True)
            along = jnp.mean(back * normal, axis=-1, keepdims=True)
            grad_hidden = grad_middle[item, rows, :] + scale * (back - shift_by - normal * along)
            grad_tokens[item, rows, :] = grad_hidden.astype(BF16)
            for turn_at in range(PASSES_MAX):
                grad_embed[turn_at:turn_at + 1, :] += jnp.sum(
                    grad_hidden * onehot[:, turn_at:turn_at + 1], axis=0, keepdims=True
                )
            return carry

        lax.fori_loop(0, span // chunk, rows_of, 0)


def finish_rows(scalars, tokens, embed_low, gain_row, grad_middle, arrived, weights):
    items, span, width = tokens.shape
    groups = len(weights)
    vmem = pl.BlockSpec(memory_space=pltpu.VMEM)
    return pl.pallas_call(
        lambda *refs: finish_kernel(groups, items, *refs),
        name="finish_rows",
        in_specs=[pl.BlockSpec(memory_space=pltpu.SMEM)] + [vmem] * (4 + (items + 1) * groups),
        out_specs=[vmem] * 3,
        out_shape=[
            jax.ShapeDtypeStruct((items, span, width), BF16),
            jax.ShapeDtypeStruct((8, width), F32),
            jax.ShapeDtypeStruct((8, width), F32),
        ],
        compiler_params=pltpu.CompilerParams(vmem_limit_bytes=VMEM_LIMIT),
        cost_estimate=pl.CostEstimate(flops=3 * 10**9, bytes_accessed=12 * 10**6, transcendentals=10**3),
    )(scalars, tokens, embed_low, gain_row, grad_middle, *sum(arrived, []), *weights)


def join_late(place, grad_out, grad_here, groups):
    rows, width = grad_out.shape
    span, columns = rows // groups, grad_here.shape[1]
    vmem = pl.BlockSpec(memory_space=pltpu.VMEM)

    def kernel(at, out, here, joined):
        joined[:, :width] = out[...]
        for shift in range(groups):
            joined[shift * span:(shift + 1) * span, width:] = here[piece_rows(at[0], groups - shift, groups, span), :]

    return pl.pallas_call(
        kernel,
        name="join_late",
        in_specs=[pl.BlockSpec(memory_space=pltpu.SMEM), vmem, vmem],
        out_specs=vmem,
        out_shape=jax.ShapeDtypeStruct((rows, width + columns), BF16),
        compiler_params=pltpu.CompilerParams(vmem_limit_bytes=VMEM_LIMIT),
        cost_estimate=pl.CostEstimate(flops=10**6, bytes_accessed=4 * 10**6, transcendentals=0),
    )(place.astype(jnp.int32)[None], grad_out, grad_here)


def assemble_late(place, late, groups, width):
    rows = late.shape[0]
    inner = width // groups
    vmem = pl.BlockSpec(memory_space=pltpu.VMEM)

    def kernel(at, late_ref, out, qkv):
        out[...] = late_ref[:, :width].astype(F32)
        for here in range(groups):

            @pl.when(at[0] == here)
            def _():
                for part in range(3):
                    row = []
                    for group in range(groups):
                        low = width + (here - group) % groups * 3 * inner + part * inner
                        row.append(late_ref[:, low:low + inner].astype(F32))
                    qkv[:, part * width:(part + 1) * width] = jnp.concatenate(row, axis=1)

    return pl.pallas_call(
        kernel,
        name="assemble_late",
        in_specs=[pl.BlockSpec(memory_space=pltpu.SMEM), vmem],
        out_specs=[vmem, vmem],
        out_shape=[jax.ShapeDtypeStruct((rows, width), F32), jax.ShapeDtypeStruct((rows, 3 * width), F32)],
        compiler_params=pltpu.CompilerParams(vmem_limit_bytes=VMEM_LIMIT),
        cost_estimate=pl.CostEstimate(flops=10**6, bytes_accessed=4 * 10**6, transcendentals=0),
    )(place.astype(jnp.int32)[None], late)


def shift_heads(piece, shift, groups):
    return lax.ppermute(piece, "heads", [(at, (at + shift) % groups) for at in range(groups)])


def swap_items(piece, bit):
    size = lax.axis_size("items")
    return lax.ppermute(piece, "items", [(at, at ^ (1 << bit)) for at in range(size)])


def item_bit(bit):
    return (lax.axis_index("items") >> bit) & 1


def halve(grad, axis, bit):
    half = grad.shape[axis] // 2
    mine = item_bit(bit)
    sent = lax.dynamic_slice_in_dim(grad, (1 - mine) * half, half, axis)
    kept = lax.dynamic_slice_in_dim(grad, mine * half, half, axis)
    return (kept.astype(F32) + swap_items(sent, bit).astype(F32)).astype(BF16)


def sum_items(grad, axis, order):
    for bit in order:
        grad = halve(grad, axis, bit)
    return grad


def gather_items(part, axis, order):
    for bit in reversed(order):
        other = swap_items(part, bit)
        high = item_bit(bit) == 1
        part = jnp.concatenate([jnp.where(high, other, part), jnp.where(high, part, other)], axis=axis)
    return part


def scatter_heads(grad, groups, static_order):
    place = lax.axis_index("heads")

    def part_for(shift):
        if static_order:
            return grad[(groups - shift) % groups]
        return lax.dynamic_index_in_dim(grad, (place + shift) % groups, 0, keepdims=False)

    parts = [part_for(0)]
    for shift in range(1, groups):
        parts.append(shift_heads(part_for(shift), shift, groups))
    return parts


def total_of(parts):
    total = parts[0].astype(F32)
    for part in parts[1:]:
        total = total + part.astype(F32)
    return total


def layer(tokens, passes, embed, gain_one, w_qkv, w_out, gain_two, w_up, w_down, cotangent):
    groups = lax.axis_size("heads")
    place = lax.axis_index("heads")
    item_count, span_here, width = tokens.shape
    row_count = item_count * span_here
    inner = width // groups
    bits = lax.axis_size("items").bit_length() - 1
    order_a = list(range(bits))
    order_b = [0] + list(range(bits - 1, 0, -1))

    belows, aboves = [], []
    for item in range(item_count):
        below, above = [], []
        low = high = tokens[item]
        for step in range(1, groups):
            low = lax.ppermute(low, "heads", [(at, at + 1) for at in range(step - 1, groups - 1)])
            high = lax.ppermute(high, "heads", [(at, at - 1) for at in range(1, groups - step + 1)])
            below.append(low)
            above.append(high)
        belows.append(below)
        aboves.append(above)

    slot_index = place * span_here + jnp.arange(span_here, dtype=jnp.int32)
    valid_len = TOK_PASS * passes
    row_mask = (slot_index[None, :] < valid_len[:, None]).astype(F32).reshape(row_count, 1)
    pass_index = (slot_index[None, :] % passes[:, None]).reshape(row_count, 1)
    onehot = (pass_index == jnp.arange(PASSES_MAX, dtype=jnp.int32)[None, :]).astype(BF16)
    w_grouped = w_qkv.T.reshape(3, groups, inner, width)

    def columns_of(shift):
        piece = lax.dynamic_index_in_dim(w_grouped, (place - shift) % groups, 1, keepdims=False)
        return piece.reshape(3 * inner, width)

    w_shifted = [columns_of(shift) for shift in range(groups)]
    out_shifted = [
        lax.dynamic_slice_in_dim(w_out, ((place - shift) % groups) * inner, inner, 0) for shift in range(groups)
    ]
    hidden = tokens.astype(F32).reshape(row_count, width) + matmul(onehot, embed)
    grad_result = cotangent.astype(F32).reshape(row_count, width) * row_mask
    grad_low = grad_result.astype(BF16)
    grad_active = matmul(grad_low, w_down.T).astype(BF16)
    embed_low = jnp.zeros((128, width), BF16).at[:PASSES_MAX].set(embed)
    gain_row = gain_one.astype(F32)[None]
    w_here = w_shifted[0].T
    w_here, w_shifted, out_shifted, grad_active = lax.optimization_barrier(
        (w_here, w_shifted, out_shifted, grad_active)
    )

    kept, mixed_parts = [], []
    for item in range(item_count):
        scalars = jnp.stack([place, passes[item]]).astype(jnp.int32)
        pieces, normed_all, qkv, lse = attention_forward(
            scalars, tokens[item], belows[item], aboves[item], embed_low, gain_row, w_here
        )
        kept.append((scalars, normed_all, qkv, lse))
        mixed_parts.append(
            jnp.concatenate([pieces[0]] + [shift_heads(pieces[s], s, groups) for s in range(1, groups)], axis=1)
        )

    mixed_rows = jnp.concatenate(mixed_parts, axis=0)
    middle = hidden + matmul(mixed_rows, jnp.concatenate(out_shifted, axis=0))
    second, norm_two_back = jax.vjp(layer_norm, middle, gain_two.astype(F32))
    second_low = second.astype(BF16)
    up_proj = matmul(second_low, w_up)
    active, gelu_back = jax.vjp(gelu_tanh, up_proj)
    active_low = active.astype(BF16)
    (grad_up,) = gelu_back(grad_active.astype(F32))
    grad_up_low = grad_up.astype(BF16)
    grad_middle_norm, grad_gain_two = norm_two_back(matmul(grad_up_low, w_up.T))
    grad_middle = grad_result + grad_middle_norm
    grad_branch = grad_middle.astype(BF16)
    grad_pieces = [
        matmul(grad_branch, out_shifted[(groups - shift) % groups].T).astype(BF16) for shift in range(groups)
    ]
    grad_pieces, active_low, second_low = lax.optimization_barrier((grad_pieces, active_low, second_low))
    for shift in range(1, groups):
        grad_pieces[shift] = shift_heads(grad_pieces[shift], shift, groups)

    grad_w_down = matmul(active_low.T, grad_low).astype(BF16)
    grad_w_up = matmul(second_low.T, grad_up_low).astype(BF16)
    share_down = halve(grad_w_down.reshape(groups, -1, width), 1, order_a[0])
    share_up = halve(grad_w_up.reshape(groups, inner, -1), 2, order_b[0])
    grad_pieces, share_down, share_up = lax.optimization_barrier((grad_pieces, share_down, share_up))
    share_down = halve(share_down, 1, order_a[1])
    share_up = halve(share_up, 2, order_b[1])

    flat_here, arrived = [], []
    for item in range(item_count):
        scalars, _, qkv, lse = kept[item]
        whole, pieces = attention_backward(
            scalars, qkv, lse, [piece[item * span_here:(item + 1) * span_here] for piece in grad_pieces]
        )
        flat_here.append(whole)
        parts = [pieces[0]]
        for shift in range(1, groups):
            parts.append(shift_heads(pieces[shift], shift, groups))
        arrived.append(parts)

    flat_here, share_down, share_up = lax.optimization_barrier((flat_here, share_down, share_up))
    share_down = sum_items(share_down, 1, order_a[2:])
    share_up = sum_items(share_up, 2, order_b[2:])
    grad_w_here = total_of(
        [matmul(entry[1].T, whole) for entry, whole in zip(kept, flat_here)]
    ).astype(BF16)
    grad_w_here, share_down, share_up, mixed_rows, active_low = lax.optimization_barrier(
        (grad_w_here, share_down, share_up, mixed_rows, active_low)
    )
    grad_w_out = matmul(mixed_rows.T, grad_branch).astype(BF16)
    share_down = total_of(scatter_heads(share_down, groups, False)).astype(BF16)
    share_up = total_of(scatter_heads(share_up, groups, False)).astype(BF16)

    late = join_late(place, grad_w_out, grad_w_here, groups)
    late = late.reshape(groups, 1 << bits, -1, width + 3 * inner)
    late = halve(late, 1, order_b[0])
    late = halve(late, 1, order_b[1])
    late = sum_items(late, 1, order_b[2:])[:, 0]
    late = scatter_heads(late, groups, True)
    down_total = gather_items(share_down, 0, order_a)
    up_total = gather_items(share_up, 1, order_b)
    out_part = total_of([part[:, :width] for part in late]).astype(BF16)
    late = jnp.concatenate([out_part] + [part[:, width:] for part in late], axis=1)[None]
    late = gather_items(late, 0, order_b).reshape(inner, -1)
    out_total, qkv_total = assemble_late(place, late, groups, width)
    grad_tokens, grad_embed, grad_gain_one = finish_rows(
        jnp.concatenate([place[None], passes]).astype(jnp.int32),
        tokens, embed_low, gain_row, grad_middle.reshape(item_count, span_here, width), arrived, w_shifted,
    )
    active_low, grad_tokens = lax.optimization_barrier((active_low, grad_tokens))
    result = middle + matmul(active_low, w_down)
    outputs = (result * row_mask).astype(BF16).reshape(item_count, span_here, width)
    small = jnp.concatenate([grad_embed[:PASSES_MAX], grad_gain_one[:1], grad_gain_two[None]], axis=0)
    small = total_of(scatter_heads(small.reshape(-1, groups, inner).transpose(1, 0, 2), groups, False))
    for bit in range(bits):
        small = small + swap_items(small, bit)
    return (
        outputs,
        grad_tokens,
        small[:PASSES_MAX],
        small[PASSES_MAX],
        qkv_total,
        out_total,
        small[PASSES_MAX + 1],
        up_total.astype(F32),
        down_total.astype(F32),
    )


def solution(mesh):
    return jax.shard_map(
        layer,
        mesh=mesh,
        in_specs=(
            P("items", "heads", None),
            P("items"),
            P(),
            P(),
            P(),
            P(),
            P(),
            P(),
            P(),
            P("items", "heads", None),
        ),
        out_specs=(
            P("items", "heads", None),
            P("items", "heads", None),
            P(None, "heads"),
            P("heads"),
            P("heads", None),
            P("heads", None),
            P("heads"),
            P("heads", None),
            P("heads", None),
        ),
        check_vma=False,
    )
```

```python
import jax
import jax.numpy as jnp
from jax import lax
from jax.experimental import pallas as pl
from jax.experimental.pallas import tpu as pltpu
from jax.sharding import PartitionSpec as P


HEAD_DIM = 64
PASSES_MAX = 5
TOK_PASS = 256

epsilon = 1e-05
masked_fill = -1e30
BF16 = jnp.bfloat16
F32 = jnp.float32
NT = (((1,), (1,)), ((), ()))
VMEM_LIMIT = 56 * 1024 * 1024


def matmul(left, right):
    return jnp.dot(left, right, preferred_element_type=F32)


def layer_norm(values_in, gain):
    centered = values_in - jnp.mean(values_in, axis=-1, keepdims=True)
    spread = jnp.mean(centered * centered, axis=-1, keepdims=True)
    return centered * lax.rsqrt(spread + epsilon) * gain


def gelu_tanh(values_in):
    return jax.nn.gelu(values_in, approximate=True)


def causal(scores_t, block):
    shape = (block, block)
    allowed = lax.broadcasted_iota(jnp.int32, shape, 0) <= lax.broadcasted_iota(jnp.int32, shape, 1)
    return jnp.where(allowed, scores_t, masked_fill)


def piece_rows(place, shift, groups, span):
    return pl.ds(pl.multiple_of(lax.rem(place + shift, groups) * span, span), span)


def forward_kernel(heads_here, groups, scalars, *refs):
    own, below, above = refs[0], refs[1:groups], refs[groups:2 * groups - 1]
    embed, gain, w_here = refs[2 * groups - 1:2 * groups + 2]
    pieces = refs[2 * groups + 2:3 * groups + 2]
    normed_out, qkv, lse, tok, vt, ot, mixed = refs[3 * groups + 2:]
    block = TOK_PASS
    full_len, _ = tok.shape
    span = full_len // groups
    blocks = full_len // block
    place, count = scalars[0], scalars[1]
    inverse = 1.0 / count.astype(F32)
    embed_rows = embed.shape[0]
    inner = heads_here * HEAD_DIM

    tok[piece_rows(place, 0, groups, span), :] = own[...]
    for step in range(1, groups):

        @pl.when(place >= step)
        def _():
            tok[piece_rows(place, groups - step, groups, span), :] = below[step - 1][...]

        @pl.when(place + step < groups)
        def _():
            tok[piece_rows(place, step, groups, span), :] = above[step - 1][...]

    def project(index, carry):
        rows = pl.ds(pl.multiple_of(index * block, block), block)
        slot = lax.broadcasted_iota(jnp.int32, (block, embed_rows), 0) + index * block
        turn = jnp.floor((slot.astype(F32) + 0.5) * inverse).astype(jnp.int32)
        pass_index = slot - turn * count
        onehot = (pass_index == lax.broadcasted_iota(jnp.int32, (block, embed_rows), 1)).astype(F32)
        hidden = tok[rows, :].astype(F32) + matmul(onehot.astype(BF16), embed[...])
        normed = layer_norm(hidden, gain[...]).astype(BF16)
        normed_out[rows, :] = normed
        projected = matmul(normed, w_here[...])
        for piece in range(3 * heads_here):
            part = projected[:, piece * HEAD_DIM:(piece + 1) * HEAD_DIM]
            if piece < heads_here:
                part = part.astype(BF16).astype(F32) * HEAD_DIM ** (-0.5)
            qkv[piece, rows, :] = part.astype(BF16)
        vt[index] = projected[:, 2 * inner:].T.astype(BF16)
        return carry

    lax.fori_loop(0, blocks, project, 0)

    for at in range(blocks):
        here = slice(at * block, (at + 1) * block)

        @pl.when(at < count)
        def _():
            def one_head(head, carry):
                query = qkv[head, here, :]
                diagonal = causal(
                    lax.dot_general(qkv[heads_here + head, here, :], query, NT, preferred_element_type=F32), block
                )
                top = jnp.max(diagonal, axis=0, keepdims=True)
                if at:
                    before = lax.dot_general(
                        qkv[heads_here + head, 0:at * block, :], query, NT, preferred_element_type=F32
                    )
                    top = jnp.maximum(top, jnp.max(before, axis=0, keepdims=True))
                weight = jnp.exp(diagonal - top)
                total = jnp.sum(weight, axis=0, keepdims=True)
                head_rows = pl.ds(pl.multiple_of(head * HEAD_DIM, HEAD_DIM), HEAD_DIM)
                out = matmul(vt[at, head_rows, :], weight.astype(BF16))
                if at:
                    weight = jnp.exp(before - top)
                    total = total + jnp.sum(weight, axis=0, keepdims=True)
                    weight = weight.astype(BF16)
                    for key_at in range(at):
                        out = out + matmul(
                            vt[key_at, head_rows, :], weight[key_at * block:(key_at + 1) * block]
                        )
                ot[head_rows, :] = out * (1.0 / total)
                lse[pl.ds(head, 1), here] = top + jnp.log(total)
                return carry

            lax.fori_loop(0, heads_here, one_head, 0)
            mixed[here, :] = ot[...].T.astype(BF16)

        @pl.when(at >= count)
        def _():
            mixed[here, :] = jnp.zeros((block, inner), BF16)

    for shift in range(groups):
        pieces[shift][...] = mixed[piece_rows(place, shift, groups, span), :]


def backward_kernel(heads_here, groups, scalars, qkv, lse, *refs):
    grad_pieces, grad_qkv, outs = refs[:groups], refs[groups], refs[groups + 1:2 * groups + 1]
    grad_heads, kt, sums, grads = refs[2 * groups + 1:]
    block = TOK_PASS
    full_len = grad_qkv.shape[0]
    span = full_len // groups
    blocks = full_len // block
    place, count = scalars[0], scalars[1]

    for shift in range(groups):
        for head in range(heads_here):
            grad_heads[head, piece_rows(place, groups - shift, groups, span), :] = grad_pieces[shift][
                :, head * HEAD_DIM:(head + 1) * HEAD_DIM
            ]

    def split(index, carry):
        rows = pl.ds(pl.multiple_of(index * block, block), block)
        for head in range(heads_here):
            kt[head, index] = qkv[heads_here + head, rows, :].astype(F32).T.astype(BF16)
        return carry

    lax.fori_loop(0, blocks, split, 0)

    def one_head(head, carry):
        sums[...] = jnp.zeros_like(sums)
        for at in range(blocks):
            here = slice(at * block, (at + 1) * block)

            @pl.when(at < count)
            def _():
                query = qkv[head, here, :]
                grad = grad_heads[head, here, :]
                row_lse = lse[pl.ds(head, 1), here]
                upto = (at + 1) * block
                keys = qkv[heads_here + head, 0:upto, :]
                values = qkv[2 * heads_here + head, 0:upto, :]
                scores = lax.dot_general(keys, query, NT, preferred_element_type=F32)
                pieces = [scores[:at * block]] if at else []
                pieces.append(causal(scores[at * block:], block))
                prob = [jnp.exp(piece - row_lse) for piece in pieces]
                back = lax.dot_general(values, grad, NT, preferred_element_type=F32)
                back = ([back[:at * block]] if at else []) + [back[at * block:]]
                inner = sum(
                    jnp.sum(one * two, axis=0, keepdims=True) for one, two in zip(prob, back)
                )
                bounds = ([(0, at * block)] if at else []) + [(at * block, upto)]
                turned = None
                for (low, high), one, two in zip(bounds, prob, back):
                    shift = (one * (two - inner)).astype(BF16)
                    sums[1, low:high, :] += matmul(one.astype(BF16), grad)
                    sums[0, low:high, :] += matmul(shift, query)
                    for key_at in range(low // block, high // block):
                        part = matmul(
                            kt[head, key_at], shift[key_at * block - low:(key_at + 1) * block - low]
                        )
                        turned = part if turned is None else turned + part
                grads[head, here, :] = (turned * HEAD_DIM ** (-0.5)).T.astype(BF16)

            @pl.when(at >= count)
            def _():
                grads[head, here, :] = jnp.zeros((block, HEAD_DIM), BF16)

        grads[heads_here + head] = sums[0].astype(BF16)
        grads[2 * heads_here + head] = sums[1].astype(BF16)
        return carry

    lax.fori_loop(0, heads_here, one_head, 0)

    def join(index, carry):
        rows = pl.ds(pl.multiple_of(index * block, block), block)
        grad_qkv[rows, :] = jnp.concatenate([grads[piece, rows, :] for piece in range(3 * heads_here)], axis=1)
        return carry

    lax.fori_loop(0, blocks, join, 0)

    for shift in range(groups):
        outs[shift][...] = grad_qkv[piece_rows(place, shift, groups, span), :]


def attention_forward(scalars, own, below, above, embed_low, gain_one, w_here):
    groups = len(below) + 1
    span, width = own.shape
    full_len = span * groups
    inner = w_here.shape[1] // 3
    heads_here = inner // HEAD_DIM
    blocks = full_len // TOK_PASS
    vmem = pl.BlockSpec(memory_space=pltpu.VMEM)
    outs = pl.pallas_call(
        lambda *refs: forward_kernel(heads_here, groups, *refs),
        name="attention_forward",
        in_specs=[pl.BlockSpec(memory_space=pltpu.SMEM)] + [vmem] * (2 * groups + 2),
        out_specs=[vmem] * (groups + 3),
        scratch_shapes=[
            pltpu.VMEM((full_len, width), BF16),
            pltpu.VMEM((blocks, inner, TOK_PASS), BF16),
            pltpu.VMEM((inner, TOK_PASS), F32),
            pltpu.VMEM((full_len, inner), BF16),
        ],
        out_shape=[jax.ShapeDtypeStruct((span, inner), BF16)] * groups
        + [
            jax.ShapeDtypeStruct((full_len, width), BF16),
            jax.ShapeDtypeStruct((3 * heads_here, full_len, HEAD_DIM), BF16),
            jax.ShapeDtypeStruct((8, full_len), F32),
        ],
        compiler_params=pltpu.CompilerParams(vmem_limit_bytes=VMEM_LIMIT),
        cost_estimate=pl.CostEstimate(flops=9 * 10**9, bytes_accessed=12 * 10**6, transcendentals=3 * 10**6),
    )(scalars, own, *below, *above, embed_low, gain_one, w_here)
    return outs[:groups], outs[groups], outs[groups + 1], outs[groups + 2]


def attention_backward(scalars, qkv, lse, grad_pieces):
    groups = len(grad_pieces)
    span, inner = grad_pieces[0].shape
    full_len = span * groups
    heads_here = inner // HEAD_DIM
    blocks = full_len // TOK_PASS
    vmem = pl.BlockSpec(memory_space=pltpu.VMEM)
    outs = pl.pallas_call(
        lambda *refs: backward_kernel(heads_here, groups, *refs),
        name="attention_backward",
        in_specs=[pl.BlockSpec(memory_space=pltpu.SMEM)] + [vmem] * (groups + 2),
        out_specs=[vmem] * (groups + 1),
        scratch_shapes=[
            pltpu.VMEM((heads_here, full_len, HEAD_DIM), BF16),
            pltpu.VMEM((heads_here, blocks, HEAD_DIM, TOK_PASS), BF16),
            pltpu.VMEM((2, full_len, HEAD_DIM), F32),
            pltpu.VMEM((3 * heads_here, full_len, HEAD_DIM), BF16),
        ],
        out_shape=[jax.ShapeDtypeStruct((full_len, 3 * inner), BF16)]
        + [jax.ShapeDtypeStruct((span, 3 * inner), BF16)] * groups,
        compiler_params=pltpu.CompilerParams(vmem_limit_bytes=VMEM_LIMIT),
        cost_estimate=pl.CostEstimate(flops=9 * 10**9, bytes_accessed=8 * 10**6, transcendentals=3 * 10**6),
    )(scalars, qkv, lse, *grad_pieces)
    return outs[0], outs[1:]


def finish_kernel(groups, items, scalars, tok, embed, gain, grad_middle, *refs):
    pieces, weights = refs[:items * groups], refs[items * groups:(items + 1) * groups]
    grad_tokens, grad_embed, grad_gain = refs[(items + 1) * groups:]
    span = tok.shape[1]
    chunk = span
    embed_rows = embed.shape[0]
    grad_embed[...] = jnp.zeros_like(grad_embed)
    grad_gain[...] = jnp.zeros_like(grad_gain)
    for item in range(items):
        count = scalars[1 + item]
        inverse = 1.0 / count.astype(F32)

        def rows_of(index, carry):
            rows = pl.ds(pl.multiple_of(index * chunk, chunk), chunk)
            slot = lax.broadcasted_iota(jnp.int32, (chunk, embed_rows), 0) + (scalars[0] * span + index * chunk)
            turn = jnp.floor((slot.astype(F32) + 0.5) * inverse).astype(jnp.int32)
            onehot = (slot - turn * count == lax.broadcasted_iota(jnp.int32, (chunk, embed_rows), 1)).astype(F32)
            hidden = tok[item, rows, :].astype(F32) + matmul(onehot.astype(BF16), embed[...])
            centered = hidden - jnp.mean(hidden, axis=-1, keepdims=True)
            scale = lax.rsqrt(jnp.mean(centered * centered, axis=-1, keepdims=True) + epsilon)
            normal = centered * scale
            back = matmul(pieces[item * groups][rows, :], weights[0][...])
            for shift in range(1, groups):
                back = back + matmul(pieces[item * groups + shift][rows, :], weights[shift][...])
            grad_gain[0:1, :] += jnp.sum(back * normal, axis=0, keepdims=True)
            back = back * gain[...]
            shift_by = jnp.mean(back, axis=-1, keepdims=True)
            along = jnp.mean(back * normal, axis=-1, keepdims=True)
            grad_hidden = grad_middle[item, rows, :] + scale * (back - shift_by - normal * along)
            grad_tokens[item, rows, :] = grad_hidden.astype(BF16)
            for turn_at in range(PASSES_MAX):
                grad_embed[turn_at:turn_at + 1, :] += jnp.sum(
                    grad_hidden * onehot[:, turn_at:turn_at + 1], axis=0, keepdims=True
                )
            return carry

        lax.fori_loop(0, span // chunk, rows_of, 0)


def finish_rows(scalars, tokens, embed_low, gain_row, grad_middle, arrived, weights):
    items, span, width = tokens.shape
    groups = len(weights)
    vmem = pl.BlockSpec(memory_space=pltpu.VMEM)
    return pl.pallas_call(
        lambda *refs: finish_kernel(groups, items, *refs),
        name="finish_rows",
        in_specs=[pl.BlockSpec(memory_space=pltpu.SMEM)] + [vmem] * (4 + (items + 1) * groups),
        out_specs=[vmem] * 3,
        out_shape=[
            jax.ShapeDtypeStruct((items, span, width), BF16),
            jax.ShapeDtypeStruct((8, width), F32),
            jax.ShapeDtypeStruct((8, width), F32),
        ],
        compiler_params=pltpu.CompilerParams(vmem_limit_bytes=VMEM_LIMIT),
        cost_estimate=pl.CostEstimate(flops=3 * 10**9, bytes_accessed=12 * 10**6, transcendentals=10**3),
    )(scalars, tokens, embed_low, gain_row, grad_middle, *sum(arrived, []), *weights)


def join_late(place, grad_out, grad_here, groups):
    rows, width = grad_out.shape
    span, columns = rows // groups, grad_here.shape[1]
    vmem = pl.BlockSpec(memory_space=pltpu.VMEM)

    def kernel(at, out, here, joined):
        joined[:, :width] = out[...]
        for shift in range(groups):
            joined[shift * span:(shift + 1) * span, width:] = here[piece_rows(at[0], groups - shift, groups, span), :]

    return pl.pallas_call(
        kernel,
        name="join_late",
        in_specs=[pl.BlockSpec(memory_space=pltpu.SMEM), vmem, vmem],
        out_specs=vmem,
        out_shape=jax.ShapeDtypeStruct((rows, width + columns), BF16),
        compiler_params=pltpu.CompilerParams(vmem_limit_bytes=VMEM_LIMIT),
        cost_estimate=pl.CostEstimate(flops=10**6, bytes_accessed=4 * 10**6, transcendentals=0),
    )(place.astype(jnp.int32)[None], grad_out, grad_here)


def assemble_late(place, late, groups, width):
    rows = late.shape[0]
    inner = width // groups
    vmem = pl.BlockSpec(memory_space=pltpu.VMEM)

    def kernel(at, late_ref, out, qkv):
        out[...] = late_ref[:, :width].astype(F32)
        for here in range(groups):

            @pl.when(at[0] == here)
            def _():
                for part in range(3):
                    row = []
                    for group in range(groups):
                        low = width + (here - group) % groups * 3 * inner + part * inner
                        row.append(late_ref[:, low:low + inner].astype(F32))
                    qkv[:, part * width:(part + 1) * width] = jnp.concatenate(row, axis=1)

    return pl.pallas_call(
        kernel,
        name="assemble_late",
        in_specs=[pl.BlockSpec(memory_space=pltpu.SMEM), vmem],
        out_specs=[vmem, vmem],
        out_shape=[jax.ShapeDtypeStruct((rows, width), F32), jax.ShapeDtypeStruct((rows, 3 * width), F32)],
        compiler_params=pltpu.CompilerParams(vmem_limit_bytes=VMEM_LIMIT),
        cost_estimate=pl.CostEstimate(flops=10**6, bytes_accessed=4 * 10**6, transcendentals=0),
    )(place.astype(jnp.int32)[None], late)


def shift_heads(piece, shift, groups):
    return lax.ppermute(piece, "heads", [(at, (at + shift) % groups) for at in range(groups)])


def swap_items(piece, bit):
    size = lax.axis_size("items")
    return lax.ppermute(piece, "items", [(at, at ^ (1 << bit)) for at in range(size)])


def item_bit(bit):
    return (lax.axis_index("items") >> bit) & 1


def halve(grad, axis, bit):
    half = grad.shape[axis] // 2
    mine = item_bit(bit)
    sent = lax.dynamic_slice_in_dim(grad, (1 - mine) * half, half, axis)
    kept = lax.dynamic_slice_in_dim(grad, mine * half, half, axis)
    return (kept.astype(F32) + swap_items(sent, bit).astype(F32)).astype(BF16)


def sum_items(grad, axis, order):
    for bit in order:
        grad = halve(grad, axis, bit)
    return grad


def gather_step(part, axis, bit):
    other = swap_items(part, bit)
    high = item_bit(bit) == 1
    return jnp.concatenate([jnp.where(high, other, part), jnp.where(high, part, other)], axis=axis)


def scatter_heads(grad, groups, static_order):
    place = lax.axis_index("heads")

    def part_for(shift):
        if static_order:
            return grad[(groups - shift) % groups]
        return lax.dynamic_index_in_dim(grad, (place + shift) % groups, 0, keepdims=False)

    parts = [part_for(0)]
    for shift in range(1, groups):
        parts.append(shift_heads(part_for(shift), shift, groups))
    return parts


def total_of(parts):
    total = parts[0].astype(F32)
    for part in parts[1:]:
        total = total + part.astype(F32)
    return total


def layer(tokens, passes, embed, gain_one, w_qkv, w_out, gain_two, w_up, w_down, cotangent):
    groups = lax.axis_size("heads")
    place = lax.axis_index("heads")
    item_count, span_here, width = tokens.shape
    row_count = item_count * span_here
    inner = width // groups
    bits = lax.axis_size("items").bit_length() - 1
    order_a = list(range(bits))
    order_b = [0] + list(range(bits - 1, 0, -1))

    belows, aboves = [], []
    for item in range(item_count):
        below, above = [], []
        low = high = tokens[item]
        for step in range(1, groups):
            low = lax.ppermute(low, "heads", [(at, at + 1) for at in range(step - 1, groups - 1)])
            high = lax.ppermute(high, "heads", [(at, at - 1) for at in range(1, groups - step + 1)])
            below.append(low)
            above.append(high)
        belows.append(below)
        aboves.append(above)

    slot_index = place * span_here + jnp.arange(span_here, dtype=jnp.int32)
    valid_len = TOK_PASS * passes
    row_mask = (slot_index[None, :] < valid_len[:, None]).astype(F32).reshape(row_count, 1)
    pass_index = (slot_index[None, :] % passes[:, None]).reshape(row_count, 1)
    onehot = (pass_index == jnp.arange(PASSES_MAX, dtype=jnp.int32)[None, :]).astype(BF16)
    w_grouped = w_qkv.T.reshape(3, groups, inner, width)

    def columns_of(shift):
        piece = lax.dynamic_index_in_dim(w_grouped, (place - shift) % groups, 1, keepdims=False)
        return piece.reshape(3 * inner, width)

    w_shifted = [columns_of(shift) for shift in range(groups)]
    out_shifted = [
        lax.dynamic_slice_in_dim(w_out, ((place - shift) % groups) * inner, inner, 0) for shift in range(groups)
    ]
    hidden = tokens.astype(F32).reshape(row_count, width) + matmul(onehot, embed)
    grad_result = cotangent.astype(F32).reshape(row_count, width) * row_mask
    grad_low = grad_result.astype(BF16)
    grad_active = matmul(grad_low, w_down.T).astype(BF16)
    embed_low = jnp.zeros((128, width), BF16).at[:PASSES_MAX].set(embed)
    gain_row = gain_one.astype(F32)[None]
    w_here = w_shifted[0].T
    w_here, w_shifted, out_shifted, grad_active = lax.optimization_barrier(
        (w_here, w_shifted, out_shifted, grad_active)
    )

    kept, mixed_parts = [], []
    for item in range(item_count):
        scalars = jnp.stack([place, passes[item]]).astype(jnp.int32)
        pieces, normed_all, qkv, lse = attention_forward(
            scalars, tokens[item], belows[item], aboves[item], embed_low, gain_row, w_here
        )
        kept.append((scalars, normed_all, qkv, lse))
        mixed_parts.append(
            jnp.concatenate([pieces[0]] + [shift_heads(pieces[s], s, groups) for s in range(1, groups)], axis=1)
        )

    mixed_rows = jnp.concatenate(mixed_parts, axis=0)
    middle = hidden + matmul(mixed_rows, jnp.concatenate(out_shifted, axis=0))
    second, norm_two_back = jax.vjp(layer_norm, middle, gain_two.astype(F32))
    second_low = second.astype(BF16)
    up_proj = matmul(second_low, w_up)
    active, gelu_back = jax.vjp(gelu_tanh, up_proj)
    active_low = active.astype(BF16)
    (grad_up,) = gelu_back(grad_active.astype(F32))
    grad_up_low = grad_up.astype(BF16)
    grad_middle_norm, grad_gain_two = norm_two_back(matmul(grad_up_low, w_up.T))
    grad_middle = grad_result + grad_middle_norm
    grad_branch = grad_middle.astype(BF16)
    grad_pieces = [
        matmul(grad_branch, out_shifted[(groups - shift) % groups].T).astype(BF16) for shift in range(groups)
    ]
    grad_pieces, active_low, second_low = lax.optimization_barrier((grad_pieces, active_low, second_low))
    for shift in range(1, groups):
        grad_pieces[shift] = shift_heads(grad_pieces[shift], shift, groups)

    grad_w_down = matmul(active_low.T, grad_low).astype(BF16)
    grad_w_up = matmul(second_low.T, grad_up_low).astype(BF16)
    share_down = halve(grad_w_down.reshape(groups, -1, width), 1, order_a[0])
    share_up = halve(grad_w_up.reshape(groups, inner, -1), 2, order_b[0])
    grad_pieces, share_down, share_up = lax.optimization_barrier((grad_pieces, share_down, share_up))
    share_down = halve(share_down, 1, order_a[1])
    share_up = halve(share_up, 2, order_b[1])

    flat_here, arrived = [], []
    for item in range(item_count):
        scalars, _, qkv, lse = kept[item]
        whole, pieces = attention_backward(
            scalars, qkv, lse, [piece[item * span_here:(item + 1) * span_here] for piece in grad_pieces]
        )
        flat_here.append(whole)
        parts = [pieces[0]]
        for shift in range(1, groups):
            parts.append(shift_heads(pieces[shift], shift, groups))
        arrived.append(parts)

    share_down = sum_items(share_down, 1, order_a[2:])
    share_up = sum_items(share_up, 2, order_b[2:])
    grad_w_here = total_of(
        [matmul(entry[1].T, whole) for entry, whole in zip(kept, flat_here)]
    ).astype(BF16)
    grad_w_here, mixed_rows = lax.optimization_barrier((grad_w_here, mixed_rows))
    grad_w_out = matmul(mixed_rows.T, grad_branch).astype(BF16)
    share_down = total_of(scatter_heads(share_down, groups, False)).astype(BF16)
    share_up = total_of(scatter_heads(share_up, groups, False)).astype(BF16)

    late = join_late(place, grad_w_out, grad_w_here, groups)
    late = late.reshape(groups, 1 << bits, -1, width + 3 * inner)
    late = halve(late, 1, order_b[0])
    late = halve(late, 1, order_b[1])
    late = sum_items(late, 1, order_b[2:])[:, 0]
    grad_tokens, grad_embed, grad_gain_one = finish_rows(
        jnp.concatenate([place[None], passes]).astype(jnp.int32),
        tokens, embed_low, gain_row, grad_middle.reshape(item_count, span_here, width), arrived, w_shifted,
    )
    result = middle + matmul(active_low, w_down)
    outputs = (result * row_mask).astype(BF16).reshape(item_count, span_here, width)
    small = jnp.concatenate([grad_embed[:PASSES_MAX], grad_gain_one[:1], grad_gain_two[None]], axis=0)
    small = scatter_heads(small.reshape(-1, groups, inner).transpose(1, 0, 2), groups, False)
    late = scatter_heads(late, groups, True)
    small, late, share_down, share_up = lax.optimization_barrier((small, late, share_down, share_up))
    small = total_of(small)
    out_part = total_of([part[:, :width] for part in late]).astype(BF16)
    late = jnp.concatenate([out_part] + [part[:, width:] for part in late], axis=1)[None]
    for at in range(bits):
        bit_a, bit_b = order_a[bits - 1 - at], order_b[bits - 1 - at]
        share_down = gather_step(share_down, 0, bit_a)
        share_up = gather_step(share_up, 1, bit_b)
        late = gather_step(late, 0, bit_b)
        small = small + swap_items(small, at)
        if at < bits - 1:
            share_down, share_up, late, small, outputs = lax.optimization_barrier(
                (share_down, share_up, late, small, outputs)
            )
    out_total, qkv_total = assemble_late(place, late.reshape(inner, -1), groups, width)
    return (
        outputs,
        grad_tokens,
        small[:PASSES_MAX],
        small[PASSES_MAX],
        qkv_total,
        out_total,
        small[PASSES_MAX + 1],
        share_up.astype(F32),
        share_down.astype(F32),
    )


def solution(mesh):
    return jax.shard_map(
        layer,
        mesh=mesh,
        in_specs=(
            P("items", "heads", None),
            P("items"),
            P(),
            P(),
            P(),
            P(),
            P(),
            P(),
            P(),
            P("items", "heads", None),
        ),
        out_specs=(
            P("items", "heads", None),
            P("items", "heads", None),
            P(None, "heads"),
            P("heads"),
            P("heads", None),
            P("heads", None),
            P("heads"),
            P("heads", None),
            P("heads", None),
        ),
        check_vma=False,
    )
```
